16 devices in a mesh: replica: 2 (over z), data: 8 (over y, x, core).
Axes of the slice: x: 2, y: 2, z: 2, core: 2. Of those that a mesh axis runs over, the one named last changes fastest.
Arguments:
- x_seq: bfloat16 [512, 16, 1024], P(('replica', 'data'))
- dy_seq: float32 [512, 16, 1024], P(('replica', 'data'))
- w_stack: bfloat16 [4, 2048, 4096], replicated
- b_stack: float32 [4, 4096], replicated
Outputs:
- output 1: float32 [4, 2048, 4096], replicated
- output 2: float32 [4, 4096], replicated
- output 3: float32 [512, 16, 1024], P(('replica', 'data'))
All inputs are finite; a program needn't handle non-finite values.
Results may differ from the reference program's by a relative error of at most 0.0150577.
Values are sent between devices in bfloat16 or wider.
A program may use at most 1 GiB of HBM per device.

```python
import jax
import jax.numpy as jnp
from jax import lax

HIDDEN = 1024
LAYERS = 4
BATCH_DEV = 32
SEQ = 16
REPLICA = 2
DATA = 8


def setup_inputs(seed: int = 0) -> dict:
    shards = REPLICA * DATA
    batch_rows = BATCH_DEV * shards
    key_list = jax.random.split(jax.random.key(seed), 4)
    x_seq = jax.random.normal(key_list[0], (batch_rows, SEQ, HIDDEN), jnp.float32).astype(jnp.bfloat16)
    dy_seq = jax.random.normal(key_list[1], (batch_rows, SEQ, HIDDEN), jnp.float32)
    w_scale = 1.5 * (2 * HIDDEN) ** -0.5
    w_stack = (jax.random.normal(key_list[2], (LAYERS, 2 * HIDDEN, 4 * HIDDEN), jnp.float32) * w_scale).astype(jnp.bfloat16)
    gate_shift = jnp.concatenate([jnp.ones((2 * HIDDEN,), jnp.float32), jnp.zeros((HIDDEN,), jnp.float32), jnp.ones((HIDDEN,), jnp.float32)])
    b_stack = gate_shift + 0.5 * jax.random.normal(key_list[3], (LAYERS, 4 * HIDDEN), jnp.float32)
    return {'x_seq': x_seq, 'dy_seq': dy_seq, 'w_stack': w_stack, 'b_stack': b_stack}


def layer_forward(u_seq, w_layer, b_layer):
    batch_rows = u_seq.shape[1]

    def time_step(carry_state, u_step):
        h_prev, c_prev = carry_state
        z_all = jnp.dot(jnp.concatenate([u_step, h_prev], axis=-1), w_layer, preferred_element_type=jnp.float32) + b_layer
        z_i, z_f, z_g, z_o = jnp.split(z_all, 4, axis=-1)
        gate_i = jax.nn.sigmoid(z_i)
        gate_f = jax.nn.sigmoid(z_f)
        gate_g = jnp.tanh(z_g)
        gate_o = jax.nn.sigmoid(z_o)
        c_new = gate_f * c_prev + gate_i * gate_g
        tanh_c = jnp.tanh(c_new)
        h_new = (gate_o * tanh_c).astype(jnp.bfloat16)
        return (h_new, c_new), (h_new, c_new, tanh_c, gate_i, gate_f, gate_g, gate_o)

    init_state = (jnp.zeros((batch_rows, HIDDEN), jnp.bfloat16), jnp.zeros((batch_rows, HIDDEN), jnp.float32))
    return lax.scan(time_step, init_state, u_seq)[1]


def layer_backward(u_seq, w_layer, saved_acts, dh_seq):
    h_seq, c_seq, tanh_seq, i_seq, f_seq, g_seq, o_seq = saved_acts
    h_prev_seq = jnp.concatenate([jnp.zeros_like(h_seq[:1]), h_seq[:-1]], axis=0)
    c_prev_seq = jnp.concatenate([jnp.zeros_like(c_seq[:1]), c_seq[:-1]], axis=0)

    def time_step(carry_state, step_in):
        dh_rec, dc_next = carry_state
        dh_out, c_prev, tanh_c, gate_i, gate_f, gate_g, gate_o = step_in
        dh_tot = dh_out + dh_rec
        dc_cur = dc_next + dh_tot * gate_o * (1.0 - tanh_c * tanh_c)
        dz_all = jnp.concatenate([dc_cur * gate_g * gate_i * (1.0 - gate_i), dc_cur * c_prev * gate_f * (1.0 - gate_f), dc_cur * gate_i * (1.0 - gate_g * gate_g), dh_tot * tanh_c * gate_o * (1.0 - gate_o)], axis=-1)
        dz_low = dz_all.astype(jnp.bfloat16)
        du_all = jnp.dot(dz_low, w_layer.T, preferred_element_type=jnp.float32)
        return (du_all[:, HIDDEN:], dc_cur * gate_f), (dz_low, du_all[:, :HIDDEN], jnp.sum(dz_all, axis=0))

    init_state = (jnp.zeros_like(dh_seq[0]), jnp.zeros_like(dh_seq[0]))
    dz_seq, dx_seq, db_steps = lax.scan(time_step, init_state, (dh_seq, c_prev_seq, tanh_seq, i_seq, f_seq, g_seq, o_seq), reverse=True)[1]
    uh_seq = jnp.concatenate([u_seq, h_prev_seq], axis=-1)
    row_count = uh_seq.shape[0] * uh_seq.shape[1]
    dw_layer = jnp.dot(uh_seq.reshape(row_count, 2 * HIDDEN).T, dz_seq.reshape(row_count, 4 * HIDDEN), preferred_element_type=jnp.float32)
    return dw_layer, jnp.sum(db_steps, axis=0), dx_seq


def shard_grads(x_rows, dy_rows, w_stack, b_stack):
    u_first = jnp.swapaxes(x_rows, 0, 1)

    def fwd_layer(u_seq, layer_in):
        saved_acts = layer_forward(u_seq, layer_in[0], layer_in[1])
        return saved_acts[0], (u_seq, saved_acts)

    layer_inputs, layer_saved = lax.scan(fwd_layer, u_first, (w_stack, b_stack))[1]

    def bwd_layer(dh_seq, layer_in):
        dw_layer, db_layer, dx_seq = layer_backward(layer_in[1], layer_in[0], layer_in[2], dh_seq)
        return dx_seq, (dw_layer, db_layer)

    dx_seq, grads = lax.scan(bwd_layer, jnp.swapaxes(dy_rows, 0, 1), (w_stack, layer_inputs, layer_saved), reverse=True)
    return grads[0], grads[1], jnp.swapaxes(dx_seq, 0, 1)


def reference(x_seq, dy_seq, w_stack, b_stack):
    shards = REPLICA * DATA
    x_parts = x_seq.reshape(shards, BATCH_DEV, SEQ, HIDDEN)
    dy_parts = dy_seq.reshape(shards, BATCH_DEV, SEQ, HIDDEN)

    def add_shard(totals, shard_in):
        dw_all, db_all, dx_rows = shard_grads(shard_in[0], shard_in[1], w_stack, b_stack)
        dw_sum = totals[0] + dw_all.astype(jnp.bfloat16).astype(jnp.float32)
        db_sum = totals[1] + db_all.astype(jnp.bfloat16).astype(jnp.float32)
        return (dw_sum, db_sum), dx_rows

    init_totals = (jnp.zeros(w_stack.shape, jnp.float32), jnp.zeros(b_stack.shape, jnp.float32))
    totals, dx_parts = lax.scan(add_shard, init_totals, (x_parts, dy_parts))
    return totals[0], totals[1], dx_parts.reshape(x_seq.shape)
```

```python
import functools

import jax
import jax.numpy as jnp
from jax import lax
from jax.experimental import pallas as pl
from jax.experimental.pallas import tpu as pltpu
from jax.sharding import PartitionSpec as P

VMEM_MAX = 67043328
BLK = 256


def sigmoid(z):
    return 0.5 * jnp.tanh(0.5 * z) + 0.5


def forward_kernel(rows, steps, hidden, x_ref, w_ref, b_ref, h_ref, gates_ref, c_ref, u_ref):
    @pl.when(pl.program_id(0) == 0)
    def _():
        u_ref[...] = x_ref[...]

    h_ref[0, :rows, :] = jnp.zeros((rows, hidden), jnp.bfloat16)
    c_ref[0, :rows, :] = jnp.zeros((rows, hidden), jnp.float32)

    @pl.loop(0, 4 * hidden // BLK)
    def _(n):
        cols = pl.ds(pl.multiple_of(n * BLK, BLK), BLK)
        part = jnp.dot(u_ref[...], w_ref[0, :hidden, cols], preferred_element_type=jnp.float32)
        gates_ref[0, :, cols] = part + b_ref[0, :, cols]

    @pl.loop(0, steps)
    def _(t):
        now = pl.ds(pl.multiple_of(t * rows, rows), rows)
        later = pl.ds(pl.multiple_of(t * rows + rows, rows), rows)
        h_prev = h_ref[0, now, :]
        for j in range(hidden // BLK):
            cols = [pl.ds(k * hidden + j * BLK, BLK) for k in range(4)]
            z = [
                gates_ref[0, now, col] + jnp.dot(h_prev, w_ref[0, hidden:, col], preferred_element_type=jnp.float32)
                for col in cols
            ]
            act = [sigmoid(z[0]), sigmoid(z[1]), jnp.tanh(z[2]), sigmoid(z[3])]
            for col, value in zip(cols, act):
                gates_ref[0, now, col] = value
            part = pl.ds(j * BLK, BLK)
            c_new = act[1] * c_ref[0, now, part] + act[0] * act[2]
            c_ref[0, later, part] = c_new
            h_ref[0, later, part] = (act[3] * jnp.tanh(c_new)).astype(jnp.bfloat16)

    u_ref[...] = h_ref[0, rows:, :]


def forward(x_rows, w_stack, b_stack, rows):
    layers, _, width = w_stack.shape
    hidden = width // 4
    total = x_rows.shape[0]
    steps = total // rows
    return pl.pallas_call(
        functools.partial(forward_kernel, rows, steps, hidden),
        grid=(layers,),
        in_specs=[
            pl.BlockSpec((total, hidden), lambda l: (0, 0)),
            pl.BlockSpec((1, 2 * hidden, width), lambda l: (l, 0, 0)),
            pl.BlockSpec((1, 1, width), lambda l: (l, 0, 0)),
        ],
        out_specs=[
            pl.BlockSpec((1, total + rows, hidden), lambda l: (l, 0, 0)),
            pl.BlockSpec((1, total, width), lambda l: (l, 0, 0)),
            pl.BlockSpec((1, total + rows, hidden), lambda l: (l, 0, 0)),
        ],
        out_shape=[
            jax.ShapeDtypeStruct((layers, total + rows, hidden), jnp.bfloat16),
            jax.ShapeDtypeStruct((layers, total, width), jnp.float32),
            jax.ShapeDtypeStruct((layers, total + rows, hidden), jnp.float32),
        ],
        scratch_shapes=[pltpu.VMEM((total, hidden), jnp.bfloat16)],
        compiler_params=pltpu.CompilerParams(vmem_limit_bytes=VMEM_MAX),
        cost_estimate=pl.CostEstimate(
            flops=2 * layers * total * 2 * hidden * width,
            bytes_accessed=2 * layers * hidden * width + 5 * 4 * layers * total * hidden,
            transcendentals=0,
        ),
        name="lstm_forward",
    )(x_rows, w_stack, b_stack.reshape(layers, 1, width))


def backward_kernel(rows, steps, hidden, e_ref, w_ref, gates_ref, c_ref, dz_ref, db_ref, wt_ref, r_ref, dc_ref):
    blocks = hidden // BLK

    @pl.loop(0, blocks)
    def _(j):
        for k in range(4):
            cols = pl.ds(pl.multiple_of(k * hidden + j * BLK, BLK), BLK)
            place = pl.ds(pl.multiple_of(j * 4 * BLK + k * BLK, BLK), BLK)
            wt_ref[place, :] = w_ref[0, :, cols].T

    r_ref[...] = jnp.zeros_like(r_ref)
    dc_ref[...] = jnp.zeros_like(dc_ref)
    db_ref[...] = jnp.zeros_like(db_ref)

    @pl.loop(0, steps)
    def _(s):
        t = steps - 1 - s
        now = pl.ds(pl.multiple_of(t * rows, rows), rows)
        later = pl.ds(pl.multiple_of(t * rows + rows, rows), rows)
        total = None
        for j in range(blocks):
            part = pl.ds(j * BLK, BLK)
            cols = [pl.ds(k * hidden + j * BLK, BLK) for k in range(4)]
            gate_i, gate_f, gate_g, gate_o = [gates_ref[0, now, col] for col in cols]
            tanh_c = jnp.tanh(c_ref[0, later, part])
            dh = e_ref[now, part] + r_ref[:, part]
            dc = dc_ref[:, part] + dh * gate_o * (1.0 - tanh_c * tanh_c)
            dz = [
                dc * gate_g * gate_i * (1.0 - gate_i),
                dc * c_ref[0, now, part] * gate_f * (1.0 - gate_f),
                dc * gate_i * (1.0 - gate_g * gate_g),
                dh * tanh_c * gate_o * (1.0 - gate_o),
            ]
            dc_ref[:, part] = dc * gate_f
            low = []
            for col, value in zip(cols, dz):
                low.append(value.astype(jnp.bfloat16))
                dz_ref[now, col] = low[-1]
                db_ref[:, col] += jnp.sum(value.reshape(rows // 8, 8, BLK), axis=0)
            back = jnp.dot(
                jnp.concatenate(low, axis=1),
                wt_ref[j * 4 * BLK : (j + 1) * 4 * BLK, :],
                preferred_element_type=jnp.float32,
            )
            total = back if total is None else total + back
        r_ref[...] = total


def backward(layer, e_rows, w_stack, gates, c_all, rows):
    _, _, width = w_stack.shape
    hidden = width // 4
    total = e_rows.shape[0]
    steps = total // rows
    return pl.pallas_call(
        functools.partial(backward_kernel, rows, steps, hidden),
        grid=(1,),
        in_specs=[
            pl.BlockSpec((total, hidden), lambda i: (0, 0), pipeline_mode=pl.Buffered(1)),
            pl.BlockSpec((1, hidden, width), lambda i: (layer, 1, 0), pipeline_mode=pl.Buffered(1)),
            pl.BlockSpec((1, total, width), lambda i: (layer, 0, 0), pipeline_mode=pl.Buffered(1)),
            pl.BlockSpec((1, total + rows, hidden), lambda i: (layer, 0, 0), pipeline_mode=pl.Buffered(1)),
        ],
        out_specs=[
            pl.BlockSpec((total, width), lambda i: (0, 0), pipeline_mode=pl.Buffered(1)),
            pl.BlockSpec((8, width), lambda i: (0, 0), pipeline_mode=pl.Buffered(1)),
        ],
        out_shape=[
            jax.ShapeDtypeStruct((total, width), jnp.bfloat16),
            jax.ShapeDtypeStruct((8, width), jnp.float32),
        ],
        scratch_shapes=[
            pltpu.VMEM((width, hidden), jnp.bfloat16),
            pltpu.VMEM((rows, hidden), jnp.float32),
            pltpu.VMEM((rows, hidden), jnp.float32),
        ],
        compiler_params=pltpu.CompilerParams(vmem_limit_bytes=VMEM_MAX),
        cost_estimate=pl.CostEstimate(
            flops=20 * 2 * total * hidden * width,
            bytes_accessed=2 * hidden * width + 7 * 4 * total * hidden,
            transcendentals=0,
        ),
        name=f"lstm_backward_{layer}",
    )(e_rows, w_stack, gates, c_all)


MESH = pl.DeviceIdType.MESH
ORDER = (7, 6, 5, 3, 4, 2, 1, 0)
AXES = ((0, 1, 2), (1, 2, 0), (2, 0, 1))


def colour_columns(width):
    tiles = width // 128
    first = -(-tiles // 3)
    second = -(-(tiles - first) // 2)
    sizes = (first * 128, second * 128, (tiles - first - second) * 128)
    return ((0, sizes[0]), (sizes[0], sizes[1]), (sizes[0] + sizes[1], sizes[2]))


def slot_one(code, axes):
    return ((code >> axes[1]) & 1) * 2 + ((code >> axes[2]) & 1)


def add_into(out_ref, a_ref, b_ref):
    @pl.loop(0, out_ref.shape[0] // 16)
    def _(i):
        at = pl.ds(pl.multiple_of(i * 16, 16), 16)
        out_ref[at, :] = a_ref[at, :] + b_ref[at, :]


def grads_kernel(
    layer, rows, hidden,
    dz_hbm, x_hbm, h_hbm, w_hbm,
    shard_ref, dx_ref,
    dz, uh, uht, w, p, r0, r1, r2, r3,
    local_sem, s0, q0, s1, q1, s2, q2, s3, q3,
):
    total, width = dz.shape
    block = 2 * hidden // 16
    me = lax.axis_index("data")
    z = lax.axis_index("replica")
    y, x, c = me // 4, lax.rem(me // 2, 2), lax.rem(me, 2)
    partner = {"replica": z, "data": y * 4 + x * 2 + 1 - c}
    across = (
        {"replica": z, "data": y * 4 + (1 - x) * 2 + c},
        {"replica": z, "data": (1 - y) * 4 + x * 2 + c},
        {"replica": 1 - z, "data": me},
    )

    u_src = x_hbm if layer == 0 else h_hbm.at[layer - 1, pl.ds(rows, total), :]
    loads = [
        pltpu.make_async_copy(u_src, uh.at[:, pl.ds(0, hidden)], local_sem.at[0]),
        pltpu.make_async_copy(h_hbm.at[layer, pl.ds(0, total), :], uh.at[:, pl.ds(hidden, hidden)], local_sem.at[1]),
        pltpu.make_async_copy(dz_hbm, dz, local_sem.at[2]),
        pltpu.make_async_copy(w_hbm.at[layer, pl.ds(0, hidden), :], w, local_sem.at[3]),
    ]
    for load in loads:
        load.start()

    barrier = pltpu.get_barrier_semaphore()
    for device in (partner,) + across:
        pl.semaphore_signal(barrier, inc=1, device_id=device, device_id_type=MESH)
    pl.semaphore_wait(barrier, 4)

    def remote(src, dst, send_sem, recv_sem, device):
        return pltpu.make_async_remote_copy(
            src_ref=src, dst_ref=dst, send_sem=send_sem, recv_sem=recv_sem, device_id=device, device_id_type=MESH
        )

    columns = colour_columns(width)
    copies = {}
    for code in range(8):
        copies[0, code] = remote(p.at[code, 1 - c], r0.at[code], s0.at[code], q0.at[code], partner)
    for k, axes in enumerate(AXES):
        cols = pl.ds(*columns[k])
        for code in range(8):
            bits = [(code >> axis) & 1 for axis in axes]
            src = p.at[code, c, :, cols]
            if bits[0]:
                slot = slot_one(code, axes)
                at = k * 4 + slot
                copies[1, k, slot] = remote(src, r1.at[slot, :, cols], s1.at[at], q1.at[at], across[axes[0]])
            elif bits[1]:
                at = k * 2 + bits[2]
                copies[2, k, bits[2]] = remote(src, r2.at[bits[2], :, cols], s2.at[at], q2.at[at], across[axes[1]])
            elif bits[2]:
                copies[3, k] = remote(src, r3.at[:, cols], s3.at[k], q3.at[k], across[axes[2]])

    loads[0].wait()
    loads[1].wait()

    @pl.loop(0, 2 * hidden // 128)
    def _(i):
        at = pl.ds(pl.multiple_of(i * 128, 128), 128)
        uht[at, :] = uh[:, at].T

    loads[2].wait()
    chunk = min(width, 1024)

    def receive_partner(code):
        copies[0, code].wait_recv()
        add_into(p.at[code, c], p.at[code, c], r0.at[code])
        for k, axes in enumerate(AXES):
            if (code >> axes[0]) & 1:
                copies[1, k, slot_one(code, axes)].start()

    before = None
    for code in ORDER:
        sides = [own + flip - 2 * own * flip for own, flip in
                 ((z, (code >> 2) & 1), (y, (code >> 1) & 1), (x, code & 1))]
        base = pl.multiple_of(((sides[0] * 2 + sides[1]) * 2 + sides[2]) * 2 * block, 2 * block)

        @pl.loop(0, width // chunk)
        def _(n):
            cols = pl.ds(pl.multiple_of(n * chunk, chunk), chunk)
            part = jnp.dot(uht[pl.ds(base, 2 * block), :], dz[:, cols], preferred_element_type=jnp.float32)
            low = part.astype(jnp.bfloat16)
            p[code, 0, :, cols] = low[:block]
            p[code, 1, :, cols] = low[block:]

        if before is not None:
            receive_partner(before)
        copies[0, code].start()
        before = code
    receive_partner(before)

    loads[3].wait()
    step = min(hidden, 512)

    @pl.loop(0, hidden // step)
    def _(n):
        at = pl.ds(pl.multiple_of(n * step, step), step)
        dx_ref[:, at] = lax.dot_general(
            dz[...], w[at, :], (((1,), (1,)), ((), ())), preferred_element_type=jnp.float32
        )

    for code in ORDER:
        for k, axes in enumerate(AXES):
            if (code >> axes[0]) & 1:
                slot = slot_one(code, axes)
                cols = pl.ds(*columns[k])
                copies[1, k, slot].wait_recv()
                here = code ^ (1 << axes[0])
                add_into(p.at[here, c, :, cols], p.at[here, c, :, cols], r1.at[slot, :, cols])
                if (here >> axes[1]) & 1:
                    copies[2, k, (here >> axes[2]) & 1].start()
    for bit in (1, 0):
        for k, axes in enumerate(AXES):
            cols = pl.ds(*columns[k])
            copies[2, k, bit].wait_recv()
            here = bit << axes[2]
            add_into(p.at[here, c, :, cols], p.at[here, c, :, cols], r2.at[bit, :, cols])
            if bit:
                copies[3, k].start()
    for k in range(3):
        cols = pl.ds(*columns[k])
        copies[3, k].wait_recv()
        add_into(shard_ref.at[:, cols], p.at[0, c, :, cols], r3.at[:, cols])
    for copy in copies.values():
        copy.wait_send()


def grads(layer, dz, x_rows, h_all, w_stack, rows):
    total, width = dz.shape
    hidden = width // 4
    block = 2 * hidden // 16
    dma = pltpu.SemaphoreType.DMA
    return pl.pallas_call(
        functools.partial(grads_kernel, layer, rows, hidden),
        in_specs=[pl.BlockSpec(memory_space=pl.ANY)] * 4,
        out_specs=[pl.BlockSpec(memory_space=pltpu.VMEM)] * 2,
        out_shape=[
            jax.ShapeDtypeStruct((block, width), jnp.bfloat16),
            jax.ShapeDtypeStruct((total, hidden), jnp.float32),
        ],
        scratch_shapes=[
            pltpu.VMEM((total, width), jnp.bfloat16),
            pltpu.VMEM((total, 2 * hidden), jnp.bfloat16),
            pltpu.VMEM((2 * hidden, total), jnp.bfloat16),
            pltpu.VMEM((hidden, width), jnp.bfloat16),
            pltpu.VMEM((8, 2, block, width), jnp.bfloat16),
            pltpu.VMEM((8, block, width), jnp.bfloat16),
            pltpu.VMEM((4, block, width), jnp.bfloat16),
            pltpu.VMEM((2, block, width), jnp.bfloat16),
            pltpu.VMEM((block, width), jnp.bfloat16),
            dma((4,)), dma((8,)), dma((8,)), dma((12,)), dma((12,)), dma((6,)), dma((6,)), dma((3,)), dma((3,)),
        ],
        compiler_params=pltpu.CompilerParams(
            collective_id=layer, has_side_effects=True, vmem_limit_bytes=VMEM_MAX
        ),
        cost_estimate=pl.CostEstimate(
            flops=6 * total * hidden * width * 5, bytes_accessed=8 * hidden * width, transcendentals=0
        ),
        name=f"lstm_grads_{layer}",
    )(dz, x_rows, h_all, w_stack)


def widen_kernel(part_ref, *refs):
    refs[-1][0] = part_ref[...].astype(jnp.float32)


def widen(total, part, layer, layers):
    height, width = part.shape
    block = min(height, 256)
    return pl.pallas_call(
        widen_kernel,
        grid=(height // block,),
        in_specs=[pl.BlockSpec((block, width), lambda i: (i, 0))]
        + ([] if total is None else [pl.BlockSpec(memory_space=pl.ANY)]),
        out_specs=pl.BlockSpec((1, block, width), lambda i: (layer, i, 0)),
        out_shape=jax.ShapeDtypeStruct((layers, height, width), jnp.float32),
        input_output_aliases={} if total is None else {1: 0},
        cost_estimate=pl.CostEstimate(flops=height * width, bytes_accessed=6 * height * width, transcendentals=0),
        name=f"widen_{layer}",
    )(*([part] if total is None else [part, total]))


def solution(mesh):
    batch_axes = ("replica", "data")

    def local_grads(x_loc, dy_loc, w_stack, b_stack):
        layers, _, width = w_stack.shape
        hidden = width // 4
        rows, steps, _ = x_loc.shape
        x_rows = jnp.swapaxes(x_loc, 0, 1).reshape(steps * rows, hidden)
        e_rows = jnp.swapaxes(dy_loc, 0, 1).reshape(steps * rows, hidden)
        h_all, gates, c_all = forward(x_rows, w_stack, b_stack, rows)
        db_list = []
        dw_sum = None
        waiting = None
        for layer in reversed(range(layers)):
            dz, db = backward(layer, e_rows, w_stack, gates, c_all, rows)
            db_list.append(jnp.sum(db, axis=0))
            shard, e_rows = grads(layer, dz, x_rows, h_all, w_stack, rows)
            if waiting is not None:
                summed, shard = lax.optimization_barrier((waiting, shard))
                dw_sum = widen(dw_sum, summed, layer + 1, layers)
            waiting = lax.all_gather(shard, batch_axes, axis=0, tiled=True)
        db_sum = lax.psum(jnp.stack(db_list[::-1]).astype(jnp.bfloat16), batch_axes).astype(jnp.float32)
        dw_sum = widen(dw_sum, waiting, 0, layers)
        dx = jnp.swapaxes(e_rows.reshape(steps, rows, hidden), 0, 1)
        return dw_sum, db_sum, dx

    return jax.shard_map(
        local_grads,
        mesh=mesh,
        in_specs=(P(batch_axes), P(batch_axes), P(), P()),
        out_specs=(P(), P(), P(batch_axes)),
        check_vma=False,
    )
```

```python
import functools

import jax
import jax.numpy as jnp
from jax import lax
from jax.experimental import pallas as pl
from jax.experimental.pallas import tpu as pltpu
from jax.sharding import PartitionSpec as P

VMEM_MAX = 67043328
BLK = 256


def sigmoid(z):
    return 0.5 * jnp.tanh(0.5 * z) + 0.5


def forward_kernel(rows, steps, hidden, x_ref, w_ref, b_ref, h_ref, gates_ref, c_ref, u_ref):
    @pl.when(pl.program_id(0) == 0)
    def _():
        u_ref[...] = x_ref[...]

    h_ref[0, :rows, :] = jnp.zeros((rows, hidden), jnp.bfloat16)
    c_ref[0, :rows, :] = jnp.zeros((rows, hidden), jnp.float32)

    @pl.loop(0, 4 * hidden // BLK)
    def _(n):
        cols = pl.ds(pl.multiple_of(n * BLK, BLK), BLK)
        part = jnp.dot(u_ref[...], w_ref[0, :hidden, cols], preferred_element_type=jnp.float32)
        gates_ref[0, :, cols] = part + b_ref[pl.ds(pl.program_id(0), 1), cols]

    @pl.loop(0, steps)
    def _(t):
        now = pl.ds(pl.multiple_of(t * rows, rows), rows)
        later = pl.ds(pl.multiple_of(t * rows + rows, rows), rows)
        h_prev = h_ref[0, now, :]
        for j in range(hidden // BLK):
            cols = [pl.ds(k * hidden + j * BLK, BLK) for k in range(4)]
            z = [
                gates_ref[0, now, col] + jnp.dot(h_prev, w_ref[0, hidden:, col], preferred_element_type=jnp.float32)
                for col in cols
            ]
            act = [sigmoid(z[0]), sigmoid(z[1]), jnp.tanh(z[2]), sigmoid(z[3])]
            for col, value in zip(cols, act):
                gates_ref[0, now, col] = value
            part = pl.ds(j * BLK, BLK)
            c_new = act[1] * c_ref[0, now, part] + act[0] * act[2]
            c_ref[0, later, part] = c_new
            h_ref[0, later, part] = (act[3] * jnp.tanh(c_new)).astype(jnp.bfloat16)

    u_ref[...] = h_ref[0, rows:, :]


def forward(x_rows, w_stack, b_stack, rows):
    layers, _, width = w_stack.shape
    hidden = width // 4
    total = x_rows.shape[0]
    steps = total // rows
    return pl.pallas_call(
        functools.partial(forward_kernel, rows, steps, hidden),
        grid=(layers,),
        in_specs=[
            pl.BlockSpec((total, hidden), lambda l: (0, 0)),
            pl.BlockSpec((1, 2 * hidden, width), lambda l: (l, 0, 0)),
            pl.BlockSpec((layers, width), lambda l: (0, 0)),
        ],
        out_specs=[
            pl.BlockSpec((1, total + rows, hidden), lambda l: (l, 0, 0)),
            pl.BlockSpec((1, total, width), lambda l: (l, 0, 0)),
            pl.BlockSpec((1, total + rows, hidden), lambda l: (l, 0, 0)),
        ],
        out_shape=[
            jax.ShapeDtypeStruct((layers, total + rows, hidden), jnp.bfloat16),
            jax.ShapeDtypeStruct((layers, total, width), jnp.float32),
            jax.ShapeDtypeStruct((layers, total + rows, hidden), jnp.float32),
        ],
        scratch_shapes=[pltpu.VMEM((total, hidden), jnp.bfloat16)],
        compiler_params=pltpu.CompilerParams(vmem_limit_bytes=VMEM_MAX),
        cost_estimate=pl.CostEstimate(
            flops=2 * layers * total * 2 * hidden * width,
            bytes_accessed=2 * layers * hidden * width + 5 * 4 * layers * total * hidden,
            transcendentals=0,
        ),
        name="lstm_forward",
    )(x_rows, w_stack, b_stack)


def backward_step(rows, hidden, t, gate, e_ref, c, wt_ref, r_ref, dc_ref, dz_ref, db_ref):
    now = pl.ds(pl.multiple_of(t * rows, rows), rows)
    later = pl.ds(pl.multiple_of(t * rows + rows, rows), rows)
    total = None
    for j in range(hidden // BLK):
        part = pl.ds(j * BLK, BLK)
        cols = [pl.ds(k * hidden + j * BLK, BLK) for k in range(4)]
        gate_i, gate_f, gate_g, gate_o = [gate(col) for col in cols]
        tanh_c = jnp.tanh(c(later, part))
        dh = e_ref[now, part] + r_ref[:, part]
        dc = dc_ref[:, part] + dh * gate_o * (1.0 - tanh_c * tanh_c)
        dz = [
            dc * gate_g * gate_i * (1.0 - gate_i),
            dc * c(now, part) * gate_f * (1.0 - gate_f),
            dc * gate_i * (1.0 - gate_g * gate_g),
            dh * tanh_c * gate_o * (1.0 - gate_o),
        ]
        dc_ref[:, part] = dc * gate_f
        low = []
        for col, value in zip(cols, dz):
            low.append(value.astype(jnp.bfloat16))
            dz_ref[now, col] = low[-1]
            db_ref[:, col] += jnp.sum(value.reshape(rows // 8, 8, BLK), axis=0)
        back = jnp.dot(
            jnp.concatenate(low, axis=1),
            wt_ref[j * 4 * BLK : (j + 1) * 4 * BLK, :],
            preferred_element_type=jnp.float32,
        )
        total = back if total is None else total + back
    r_ref[...] = total


def transpose_recurrent(hidden, w, wt_ref):
    @pl.loop(0, hidden // BLK)
    def _(j):
        for k in range(4):
            cols = pl.ds(pl.multiple_of(k * hidden + j * BLK, BLK), BLK)
            place = pl.ds(pl.multiple_of(j * 4 * BLK + k * BLK, BLK), BLK)
            wt_ref[place, :] = w(cols).T


def backward_kernel(rows, steps, hidden, e_ref, w_ref, gates_ref, c_ref, dz_ref, db_ref, wt_ref, r_ref, dc_ref):
    transpose_recurrent(hidden, lambda cols: w_ref[0, :, cols], wt_ref)
    r_ref[...] = jnp.zeros_like(r_ref)
    dc_ref[...] = jnp.zeros_like(dc_ref)
    db_ref[...] = jnp.zeros_like(db_ref)

    @pl.loop(0, steps)
    def _(s):
        t = steps - 1 - s
        now = pl.ds(pl.multiple_of(t * rows, rows), rows)
        backward_step(
            rows, hidden, t, lambda col: gates_ref[0, now, col], e_ref, lambda at, col: c_ref[0, at, col],
            wt_ref, r_ref, dc_ref, dz_ref, db_ref,
        )


def backward(layer, e_rows, w_stack, gates, c_all, rows):
    _, _, width = w_stack.shape
    hidden = width // 4
    total = e_rows.shape[0]
    steps = total // rows
    return pl.pallas_call(
        functools.partial(backward_kernel, rows, steps, hidden),
        grid=(1,),
        in_specs=[
            pl.BlockSpec((total, hidden), lambda i: (0, 0), pipeline_mode=pl.Buffered(1)),
            pl.BlockSpec((1, hidden, width), lambda i: (layer, 1, 0), pipeline_mode=pl.Buffered(1)),
            pl.BlockSpec((1, total, width), lambda i: (layer, 0, 0), pipeline_mode=pl.Buffered(1)),
            pl.BlockSpec((1, total + rows, hidden), lambda i: (layer, 0, 0), pipeline_mode=pl.Buffered(1)),
        ],
        out_specs=[
            pl.BlockSpec((total, width), lambda i: (0, 0), pipeline_mode=pl.Buffered(1)),
            pl.BlockSpec((8, width), lambda i: (0, 0), pipeline_mode=pl.Buffered(1)),
        ],
        out_shape=[
            jax.ShapeDtypeStruct((total, width), jnp.bfloat16),
            jax.ShapeDtypeStruct((8, width), jnp.float32),
        ],
        scratch_shapes=[
            pltpu.VMEM((width, hidden), jnp.bfloat16),
            pltpu.VMEM((rows, hidden), jnp.float32),
            pltpu.VMEM((rows, hidden), jnp.float32),
        ],
        compiler_params=pltpu.CompilerParams(vmem_limit_bytes=VMEM_MAX),
        cost_estimate=pl.CostEstimate(
            flops=20 * 2 * total * hidden * width,
            bytes_accessed=2 * hidden * width + 7 * 4 * total * hidden,
            transcendentals=0,
        ),
        name=f"lstm_backward_{layer}",
    )(e_rows, w_stack, gates, c_all)


MESH = pl.DeviceIdType.MESH
ORDER = (7, 6, 5, 3, 4, 2, 1, 0)
AXES = ((0, 1, 2), (1, 2, 0), (2, 0, 1))


def colour_columns(width):
    tiles = width // 128
    first = -(-tiles // 3)
    second = -(-(tiles - first) // 2)
    sizes = (first * 128, second * 128, (tiles - first - second) * 128)
    return ((0, sizes[0]), (sizes[0], sizes[1]), (sizes[0] + sizes[1], sizes[2]))


def slot_one(code, axes):
    return ((code >> axes[1]) & 1) * 2 + ((code >> axes[2]) & 1)


def add_into(out_ref, a_ref, b_ref):
    @pl.loop(0, out_ref.shape[0] // 16)
    def _(i):
        at = pl.ds(pl.multiple_of(i * 16, 16), 16)
        out_ref[at, :] = a_ref[at, :] + b_ref[at, :]


def grads_kernel(layer, rows, hidden, dz_hbm, db_hbm, x_hbm, h_hbm, w_hbm, gates_hbm, c_hbm, *refs):
    below = layer - 1
    if layer:
        shard_ref, dbsum_ref, dz_out, db_ref, *refs = refs
        dz, uh, uht, w, p, r0, r1, r2, r3, db8, part_db, got_db, *refs = refs
        local_sem, s0, q0, s1, q1, s2, q2, s3, q3, sd, qd, *refs = refs
        dx_ref, c_all, ring, r_ref, dc_ref, ring_sem = refs
    else:
        shard_ref, dbsum_ref, dx_ref, *refs = refs
        dz, uh, uht, w, p, r0, r1, r2, r3, db8, part_db, got_db, *refs = refs
        local_sem, s0, q0, s1, q1, s2, q2, s3, q3, sd, qd = refs
    total, width = dz.shape
    steps = total // rows
    block = 2 * hidden // 16
    parts = width // hidden
    me = lax.axis_index("data")
    z = lax.axis_index("replica")
    y, x, c = me // 4, lax.rem(me // 2, 2), lax.rem(me, 2)
    partner = {"replica": z, "data": y * 4 + x * 2 + 1 - c}
    across = (
        {"replica": z, "data": y * 4 + (1 - x) * 2 + c},
        {"replica": z, "data": (1 - y) * 4 + x * 2 + c},
        {"replica": 1 - z, "data": me},
    )

    u_src = x_hbm if layer == 0 else h_hbm.at[below, pl.ds(rows, total), :]
    loads = [
        pltpu.make_async_copy(u_src, uh.at[:, pl.ds(0, hidden)], local_sem.at[0]),
        pltpu.make_async_copy(h_hbm.at[layer, pl.ds(0, total), :], uh.at[:, pl.ds(hidden, hidden)], local_sem.at[1]),
        pltpu.make_async_copy(dz_hbm, dz, local_sem.at[2]),
        pltpu.make_async_copy(db_hbm, db8, local_sem.at[3]),
        pltpu.make_async_copy(w_hbm.at[layer, pl.ds(0, hidden), :], w, local_sem.at[4]),
    ]
    if layer:
        loads.append(pltpu.make_async_copy(c_hbm.at[below], c_all, local_sem.at[5]))
    for load in loads:
        load.start()

    def gates_load(s, slot):
        at = pl.ds(pl.multiple_of((steps - 1 - s) * rows, rows), rows)
        return pltpu.make_async_copy(gates_hbm.at[below, at, :], ring.at[slot], ring_sem.at[slot])

    depth = 4
    if layer:
        for s in range(min(depth, steps)):
            gates_load(s, s).start()

    barrier = pltpu.get_barrier_semaphore()
    for device in (partner,) + across:
        pl.semaphore_signal(barrier, inc=1, device_id=device, device_id_type=MESH)
    pl.semaphore_wait(barrier, 4)

    def remote(src, dst, send_sem, recv_sem, device):
        return pltpu.make_async_remote_copy(
            src_ref=src, dst_ref=dst, send_sem=send_sem, recv_sem=recv_sem, device_id=device, device_id_type=MESH
        )

    columns = colour_columns(width)
    copies = {}
    for code in range(8):
        for n in range(parts):
            at = code * parts + n
            src = p.at[code, 1 - c, :, pl.ds(n * hidden, hidden)]
            copies[0, code, n] = remote(src, r0.at[pl.ds(at * block, block), :], s0.at[at], q0.at[at], partner)
    for k, axes in enumerate(AXES):
        cols = pl.ds(*columns[k])
        for code in range(8):
            bits = [(code >> axis) & 1 for axis in axes]
            src = p.at[code, c, :, cols]
            if bits[0]:
                slot = slot_one(code, axes)
                at = k * 4 + slot
                copies[1, k, slot] = remote(src, r1.at[slot, :, cols], s1.at[at], q1.at[at], across[axes[0]])
            elif bits[1]:
                at = k * 2 + bits[2]
                copies[2, k, bits[2]] = remote(src, r2.at[bits[2], :, cols], s2.at[at], q2.at[at], across[axes[1]])
            elif bits[2]:
                copies[3, k] = remote(src, r3.at[:, cols], s3.at[k], q3.at[k], across[axes[2]])
    for stage, device in enumerate((partner,) + across):
        copies[4, stage] = remote(part_db.at[stage], got_db.at[stage], sd.at[stage], qd.at[stage], device)

    def bias_stage(stage):
        copies[4, stage].wait_recv()
        out = part_db.at[stage + 1] if stage < 3 else dbsum_ref
        out[...] = part_db[stage] + got_db[stage]
        if stage < 3:
            copies[4, stage + 1].start()

    loads[3].wait()
    part_db[0] = jnp.sum(db8[...], axis=0, keepdims=True).astype(jnp.bfloat16).astype(jnp.float32)
    loads[0].wait()
    loads[1].wait()

    @pl.loop(0, 2 * hidden // 128)
    def _(i):
        at = pl.ds(pl.multiple_of(i * 128, 128), 128)
        uht[at, :] = uh[:, at].T

    copies[4, 0].start()
    loads[2].wait()
    chunk = min(width, 1024)

    def receive_partner(code):
        for n in range(parts):
            copies[0, code, n].wait_recv()
            cols = pl.ds(n * hidden, hidden)
            mine = p.at[code, c, :, cols]
            add_into(mine, mine, r0.at[pl.ds((code * parts + n) * block, block), :])
        for k, axes in enumerate(AXES):
            if (code >> axes[0]) & 1:
                copies[1, k, slot_one(code, axes)].start()

    before = None
    for code in ORDER:
        sides = [
            own + flip - 2 * own * flip
            for own, flip in ((z, (code >> 2) & 1), (y, (code >> 1) & 1), (x, code & 1))
        ]
        base = pl.multiple_of(((sides[0] * 2 + sides[1]) * 2 + sides[2]) * 2 * block, 2 * block)

        @pl.loop(0, width // chunk)
        def _(n):
            cols = pl.ds(pl.multiple_of(n * chunk, chunk), chunk)
            part = jnp.dot(uht[pl.ds(base, 2 * block), :], dz[:, cols], preferred_element_type=jnp.float32)
            low = part.astype(jnp.bfloat16)
            p[code, 0, :, cols] = low[:block]
            p[code, 1, :, cols] = low[block:]

        if before is not None:
            receive_partner(before)
        for n in range(parts):
            copies[0, code, n].start()
        before = code
    receive_partner(before)
    bias_stage(0)

    loads[4].wait()
    step = min(hidden, 512)

    @pl.loop(0, hidden // step)
    def _(n):
        at = pl.ds(pl.multiple_of(n * step, step), step)
        dx_ref[:, at] = lax.dot_general(
            dz[...], w[at, :], (((1,), (1,)), ((), ())), preferred_element_type=jnp.float32
        )

    def first_crossing(codes):
        for code in codes:
            for k, axes in enumerate(AXES):
                if (code >> axes[0]) & 1:
                    slot = slot_one(code, axes)
                    cols = pl.ds(*columns[k])
                    copies[1, k, slot].wait_recv()
                    here = code ^ (1 << axes[0])
                    mine = p.at[here, c, :, cols]
                    add_into(mine, mine, r1.at[slot, :, cols])
                    if (here >> axes[1]) & 1:
                        copies[2, k, (here >> axes[2]) & 1].start()

    bias_stage(1)
    if layer:
        reload = pltpu.make_async_copy(w_hbm.at[below, pl.ds(hidden, hidden), :], w, local_sem.at[4])
        reload.start()
        r_ref[...] = jnp.zeros_like(r_ref)
        dc_ref[...] = jnp.zeros_like(dc_ref)
        db_ref[...] = jnp.zeros_like(db_ref)
        loads[5].wait()
        reload.wait()
        transpose_recurrent(hidden, lambda cols: w[:, cols], r0)

        @pl.loop(0, steps)
        def _(s):
            slot = lax.rem(s, depth)
            gates_load(s, slot).wait()
            backward_step(
                rows, hidden, steps - 1 - s, lambda col: ring[slot, :, col], dx_ref,
                lambda at, col: c_all[at, col], r0, r_ref, dc_ref, dz, db_ref,
            )

            @pl.when(s + depth < steps)
            def _():
                gates_load(s + depth, slot).start()

            @pl.when(s == steps // 2 - 2)
            def _():
                first_crossing(ORDER[:1])

            @pl.when(s == steps - 3)
            def _():
                first_crossing(ORDER[1:4])

        store = pltpu.make_async_copy(dz, dz_out, local_sem.at[2])
        store.start()
        first_crossing(ORDER[4:])
    else:
        first_crossing(ORDER)
    bias_stage(2)
    for bit in (1, 0):
        for k, axes in enumerate(AXES):
            cols = pl.ds(*columns[k])
            copies[2, k, bit].wait_recv()
            mine = p.at[bit << axes[2], c, :, cols]
            add_into(mine, mine, r2.at[bit, :, cols])
            if bit:
                copies[3, k].start()
    bias_stage(3)
    for k in range(3):
        cols = pl.ds(*columns[k])
        copies[3, k].wait_recv()
        add_into(shard_ref.at[:, cols], p.at[0, c, :, cols], r3.at[:, cols])
    for copy in copies.values():
        copy.wait_send()
    if layer:
        store.wait()


def grads(layer, dz, db, x_rows, h_all, w_stack, gates, c_all, rows):
    total, width = dz.shape
    hidden = width // 4
    block = 2 * hidden // 16
    parts = 8 * (width // hidden)
    dma = pltpu.SemaphoreType.DMA
    vmem = pl.BlockSpec(memory_space=pltpu.VMEM)
    hbm = pl.BlockSpec(memory_space=pl.ANY)
    out_shape = [
        jax.ShapeDtypeStruct((block, width), jnp.bfloat16),
        jax.ShapeDtypeStruct((1, width), jnp.float32),
    ]
    scratch = [
        pltpu.VMEM((total, width), jnp.bfloat16),
        pltpu.VMEM((total, 2 * hidden), jnp.bfloat16),
        pltpu.VMEM((2 * hidden, total), jnp.bfloat16),
        pltpu.VMEM((hidden, width), jnp.bfloat16),
        pltpu.VMEM((8, 2, block, width), jnp.bfloat16),
        pltpu.VMEM((width, hidden), jnp.bfloat16),
        pltpu.VMEM((4, block, width), jnp.bfloat16),
        pltpu.VMEM((2, block, width), jnp.bfloat16),
        pltpu.VMEM((block, width), jnp.bfloat16),
        pltpu.VMEM((8, width), jnp.float32),
        pltpu.VMEM((4, 1, width), jnp.float32),
        pltpu.VMEM((4, 1, width), jnp.float32),
        dma((6,)), dma((parts,)), dma((parts,)), dma((12,)), dma((12,)), dma((6,)), dma((6,)), dma((3,)), dma((3,)),
        dma((4,)), dma((4,)),
    ]
    if layer:
        out_specs = [vmem, vmem, hbm, vmem]
        out_shape += [
            jax.ShapeDtypeStruct((total, width), jnp.bfloat16),
            jax.ShapeDtypeStruct((8, width), jnp.float32),
        ]
        scratch += [
            pltpu.VMEM((total, hidden), jnp.float32),
            pltpu.VMEM((total + rows, hidden), jnp.float32),
            pltpu.VMEM((4, rows, width), jnp.float32),
            pltpu.VMEM((rows, hidden), jnp.float32),
            pltpu.VMEM((rows, hidden), jnp.float32),
            dma((4,)),
        ]
    else:
        out_specs = [vmem, vmem, vmem]
        out_shape += [jax.ShapeDtypeStruct((total, hidden), jnp.float32)]
    return pl.pallas_call(
        functools.partial(grads_kernel, layer, rows, hidden),
        in_specs=[hbm] * 7,
        out_specs=out_specs,
        out_shape=out_shape,
        scratch_shapes=scratch,
        compiler_params=pltpu.CompilerParams(
            collective_id=layer, has_side_effects=True, vmem_limit_bytes=VMEM_MAX
        ),
        cost_estimate=pl.CostEstimate(
            flops=6 * total * hidden * width * 5, bytes_accessed=8 * hidden * width, transcendentals=0
        ),
        name=f"lstm_grads_{layer}",
    )(dz, db, x_rows, h_all, w_stack, gates, c_all)


def widen_kernel(part_ref, *refs):
    refs[-1][0] = part_ref[...].astype(jnp.float32)


def widen(total, part, layer, layers):
    height, width = part.shape
    block = min(height, 256)
    return pl.pallas_call(
        widen_kernel,
        grid=(height // block,),
        in_specs=[pl.BlockSpec((block, width), lambda i: (i, 0))]
        + ([] if total is None else [pl.BlockSpec(memory_space=pl.ANY)]),
        out_specs=pl.BlockSpec((1, block, width), lambda i: (layer, i, 0)),
        out_shape=jax.ShapeDtypeStruct((layers, height, width), jnp.float32),
        input_output_aliases={} if total is None else {1: 0},
        cost_estimate=pl.CostEstimate(flops=height * width, bytes_accessed=6 * height * width, transcendentals=0),
        name=f"widen_{layer}",
    )(*([part] if total is None else [part, total]))


def solution(mesh):
    batch_axes = ("replica", "data")

    def local_grads(x_loc, dy_loc, w_stack, b_stack):
        layers, _, width = w_stack.shape
        hidden = width // 4
        rows, steps, _ = x_loc.shape
        x_rows = jnp.swapaxes(x_loc, 0, 1).reshape(steps * rows, hidden)
        e_rows = jnp.swapaxes(dy_loc, 0, 1).reshape(steps * rows, hidden)
        h_all, gates, c_all = forward(x_rows, w_stack, b_stack, rows)
        db_list = []
        dw_sum = None
        waiting = None
        dz, db = backward(layers - 1, e_rows, w_stack, gates, c_all, rows)
        for layer in reversed(range(layers)):
            shard, db_sum, *rest = grads(layer, dz, db, x_rows, h_all, w_stack, gates, c_all, rows)
            if layer:
                dz, db = rest
            db_list.append(db_sum)
            if waiting is not None:
                summed, shard = lax.optimization_barrier((waiting, shard))
                dw_sum = widen(dw_sum, summed, layer + 1, layers)
            waiting = lax.all_gather(shard, batch_axes, axis=0, tiled=True)
        e_rows = rest[0]
        db_sum = jnp.concatenate(db_list[::-1], axis=0)
        dw_sum = widen(dw_sum, waiting, 0, layers)
        dx = jnp.swapaxes(e_rows.reshape(steps, rows, hidden), 0, 1)
        return dw_sum, db_sum, dx

    return jax.shard_map(
        local_grads,
        mesh=mesh,
        in_specs=(P(batch_axes), P(batch_axes), P(), P()),
        out_specs=(P(), P(), P(batch_axes)),
        check_vma=False,
    )
```

```python
import functools

import jax
import jax.numpy as jnp
from jax import lax
from jax.experimental import pallas as pl
from jax.experimental.pallas import tpu as pltpu
from jax.sharding import PartitionSpec as P

VMEM_MAX = 67043328
BLK = 256


def sigmoid(z):
    return 0.5 * jnp.tanh(0.5 * z) + 0.5


def forward_kernel(
    rows, x_hbm, w_hbm, b_ref, h_out, gates_out, c_out,
    h, gates, c, w_in, w_rec, x_sem, first_sem, in_sem, rec_sem, store_sem,
):
    layers, width = b_ref.shape
    hidden = width // 4
    total = gates.shape[1]
    steps = total // rows
    span = total // 4
    group = steps // 4

    def load_in(l, slot):
        return pltpu.make_async_copy(w_hbm.at[l, pl.ds(0, hidden), :], w_in.at[slot], in_sem.at[slot])

    def load_rec(l, slot):
        return pltpu.make_async_copy(w_hbm.at[l, pl.ds(hidden, hidden), :], w_rec.at[slot], rec_sem.at[slot])

    def load_first(k):
        cols = pl.ds(k * hidden, hidden)
        return pltpu.make_async_copy(w_hbm.at[0, pl.ds(0, hidden), cols], w_in.at[0, :, cols], first_sem.at[k])

    def stores(l, slot, t):
        now = pl.ds(pl.multiple_of(t * rows, rows), rows)
        later = pl.ds(pl.multiple_of(t * rows + rows, rows), rows)
        return [
            pltpu.make_async_copy(gates.at[slot, now, :], gates_out.at[l, now, :], store_sem.at[slot, 0]),
            pltpu.make_async_copy(h.at[slot, later, :], h_out.at[l, later, :], store_sem.at[slot, 1]),
            pltpu.make_async_copy(c.at[slot, later, :], c_out.at[l, later, :], store_sem.at[slot, 2]),
        ]

    def zero_stores(l, slot):
        at = pl.ds(0, rows)
        return [
            pltpu.make_async_copy(h.at[slot, at, :], h_out.at[l, at, :], store_sem.at[slot, 1]),
            pltpu.make_async_copy(c.at[slot, at, :], c_out.at[l, at, :], store_sem.at[slot, 2]),
        ]

    def finish_stores(l, slot):
        for copy in zero_stores(l, slot):
            copy.wait()

        @pl.loop(0, steps)
        def _(t):
            for copy in stores(l, slot, t):
                copy.wait()

    x_load = pltpu.make_async_copy(x_hbm, h.at[1, pl.ds(rows, total), :], x_sem)
    x_load.start()
    for k in range(4):
        load_first(k).start()
    load_rec(0, 0).start()
    load_in(1, 1).start()
    for slot in range(2):
        h[slot, :rows, :] = jnp.zeros((rows, hidden), jnp.bfloat16)
        c[slot, :rows, :] = jnp.zeros((rows, hidden), jnp.float32)
    x_load.wait()
    for k in range(4):
        load_first(k).wait()

        @pl.loop(0, hidden // BLK)
        def _(n):
            cols = pl.ds(pl.multiple_of(k * hidden + n * BLK, BLK), BLK)
            part = jnp.dot(h[1, rows : rows + 3 * span, :], w_in[0, :, cols], preferred_element_type=jnp.float32)
            gates[0, : 3 * span, cols] = part + b_ref[0:1, cols]

    @pl.loop(0, layers)
    def _(l):
        slot = lax.rem(l, 2)
        other = 1 - slot

        @pl.when(l + 1 < layers)
        def _():
            load_rec(l + 1, other).start()

        for copy in zero_stores(l, slot):
            copy.start()
        load_rec(l, slot).wait()

        @pl.when((l > 0) & (l + 1 < layers))
        def _():
            load_in(l + 1, other).wait()

        @pl.when(l == 0)
        def _():
            load_in(1, 1).wait()

        @pl.loop(0, steps)
        def _(t):
            now = pl.ds(pl.multiple_of(t * rows, rows), rows)
            later = pl.ds(pl.multiple_of(t * rows + rows, rows), rows)
            h_prev = h[slot, now, :]
            for j in range(hidden // BLK):
                cols = [pl.ds(k * hidden + j * BLK, BLK) for k in range(4)]
                z = [
                    gates[slot, now, col]
                    + jnp.dot(h_prev, w_rec[slot, :, col], preferred_element_type=jnp.float32)
                    for col in cols
                ]
                if j == hidden // BLK - 1:
                    early = t < group
                    source = jnp.where(early, other, slot)
                    target = jnp.where(early, slot, other)
                    row = pl.multiple_of(jnp.where(early, 3, t // group - 1) * span, span)
                    bias = jnp.minimum(jnp.where(early, l, l + 1), layers - 1)
                    u = h[source, pl.ds(pl.multiple_of(row + rows, rows), span), :]
                    for i in range(width // group // BLK):
                        col = pl.ds(pl.multiple_of(lax.rem(t, group) * (width // group) + i * BLK, BLK), BLK)
                        gates[target, pl.ds(row, span), col] = b_ref[pl.ds(bias, 1), col] + jnp.dot(
                            u, w_in[target, :, col], preferred_element_type=jnp.float32
                        )
                act = [sigmoid(z[0]), sigmoid(z[1]), jnp.tanh(z[2]), sigmoid(z[3])]
                for col, value in zip(cols, act):
                    gates[slot, now, col] = value
                part = pl.ds(j * BLK, BLK)
                c_new = act[1] * c[slot, now, part] + act[0] * act[2]
                c[slot, later, part] = c_new
                h[slot, later, part] = (act[3] * jnp.tanh(c_new)).astype(jnp.bfloat16)

            @pl.when(t > 0)
            def _():
                for copy in stores(l, slot, t - 1):
                    copy.start()

            @pl.when(t == group - 1)
            def _():
                @pl.when(l > 0)
                def _():
                    finish_stores(l - 1, other)

                @pl.when(l + 2 < layers)
                def _():
                    load_in(l + 2, slot).start()

        for copy in stores(l, slot, steps - 1):
            copy.start()

    finish_stores(layers - 1, (layers - 1) % 2)


def forward(x_rows, w_stack, b_stack, rows):
    layers, _, width = w_stack.shape
    hidden = width // 4
    total = x_rows.shape[0]
    dma = pltpu.SemaphoreType.DMA
    hbm = pl.BlockSpec(memory_space=pl.ANY)
    return pl.pallas_call(
        functools.partial(forward_kernel, rows),
        in_specs=[hbm, hbm, pl.BlockSpec(memory_space=pltpu.VMEM)],
        out_specs=[hbm] * 3,
        out_shape=[
            jax.ShapeDtypeStruct((layers, total + rows, hidden), jnp.bfloat16),
            jax.ShapeDtypeStruct((layers, total, width), jnp.float32),
            jax.ShapeDtypeStruct((layers, total + rows, hidden), jnp.float32),
        ],
        scratch_shapes=[
            pltpu.VMEM((2, total + rows, hidden), jnp.bfloat16),
            pltpu.VMEM((2, total, width), jnp.float32),
            pltpu.VMEM((2, total + rows, hidden), jnp.float32),
            pltpu.VMEM((2, hidden, width), jnp.bfloat16),
            pltpu.VMEM((2, hidden, width), jnp.bfloat16),
            dma, dma((4,)), dma((2,)), dma((2,)), dma((2, 3)),
        ],
        compiler_params=pltpu.CompilerParams(vmem_limit_bytes=VMEM_MAX),
        cost_estimate=pl.CostEstimate(
            flops=2 * layers * total * 2 * hidden * width,
            bytes_accessed=2 * layers * hidden * width + 5 * 4 * layers * total * hidden,
            transcendentals=0,
        ),
        name="lstm_forward",
    )(x_rows, w_stack, b_stack)


def backward_step(rows, hidden, t, gate, e, c, wt_ref, r_ref, dc_ref, dz_ref, db_ref):
    now = pl.ds(pl.multiple_of(t * rows, rows), rows)
    later = pl.ds(pl.multiple_of(t * rows + rows, rows), rows)
    total = None
    for j in range(hidden // BLK):
        part = pl.ds(j * BLK, BLK)
        cols = [pl.ds(k * hidden + j * BLK, BLK) for k in range(4)]
        gate_i, gate_f, gate_g, gate_o = [gate(col) for col in cols]
        tanh_c = jnp.tanh(c(later, part))
        dh = e(part) + r_ref[:, part]
        dc = dc_ref[:, part] + dh * gate_o * (1.0 - tanh_c * tanh_c)
        dz = [
            dc * gate_g * gate_i * (1.0 - gate_i),
            dc * c(now, part) * gate_f * (1.0 - gate_f),
            dc * gate_i * (1.0 - gate_g * gate_g),
            dh * tanh_c * gate_o * (1.0 - gate_o),
        ]
        dc_ref[:, part] = dc * gate_f
        low = []
        for col, value in zip(cols, dz):
            low.append(value.astype(jnp.bfloat16))
            dz_ref[now, col] = low[-1]
            db_ref[:, col] += jnp.sum(value.reshape(rows // 8, 8, BLK), axis=0)
        back = jnp.dot(
            jnp.concatenate(low, axis=1),
            wt_ref[j * 4 * BLK : (j + 1) * 4 * BLK, :],
            preferred_element_type=jnp.float32,
        )
        total = back if total is None else total + back
    r_ref[...] = total


def transpose_gate(hidden, k, w_ref, wt_ref):
    @pl.loop(0, hidden // BLK)
    def _(j):
        cols = pl.ds(pl.multiple_of(k * hidden + j * BLK, BLK), BLK)
        place = pl.ds(pl.multiple_of(j * 4 * BLK + k * BLK, BLK), BLK)
        wt_ref[place, :] = w_ref[:, cols].T


def backward_kernel(
    layer, rows, steps, hidden, e_hbm, w_hbm, gates_hbm, c_hbm, dz_out, db_ref,
    e_all, w, c_all, ring, dz, wt_ref, r_ref, dc_ref, w_sem, ring_sem, out_sem, sem,
):
    depth = ring.shape[0]

    def gates_load(s, slot):
        at = pl.ds(pl.multiple_of((steps - 1 - s) * rows, rows), rows)
        return pltpu.make_async_copy(gates_hbm.at[layer, at, :], ring.at[slot], ring_sem.at[slot])

    def store(s):
        at = pl.ds(pl.multiple_of((steps - 1 - s) * rows, rows), rows)
        return pltpu.make_async_copy(dz.at[at, :], dz_out.at[at, :], out_sem)

    def e_step(t, col):
        first, count = col.start // 128, col.size // 128
        at = pl.ds(t, rows, stride=steps)
        return jnp.concatenate([e_all[first + i, at, :] for i in range(count)], axis=1)

    def w_load(k):
        cols = pl.ds(k * hidden, hidden)
        return pltpu.make_async_copy(w_hbm.at[layer, pl.ds(hidden, hidden), cols], w.at[:, cols], w_sem.at[k])

    tiles = hidden // 128
    loads = [pltpu.make_async_copy(c_hbm.at[layer], c_all, sem.at[tiles])]
    for i in range(tiles):
        loads.append(pltpu.make_async_copy(e_hbm.at[:, pl.ds(i * 128, 128)], e_all.at[i], sem.at[i]))
    for k in range(4):
        w_load(k).start()
    for load in loads:
        load.start()
    for s in range(min(depth, steps)):
        gates_load(s, s).start()
    r_ref[...] = jnp.zeros_like(r_ref)
    dc_ref[...] = jnp.zeros_like(dc_ref)
    db_ref[...] = jnp.zeros_like(db_ref)
    for k in range(4):
        w_load(k).wait()
        transpose_gate(hidden, k, w, wt_ref)
    for load in loads:
        load.wait()

    @pl.loop(0, steps)
    def _(s):
        t = steps - 1 - s
        slot = lax.rem(s, depth)
        gates_load(s, slot).wait()
        backward_step(
            rows, hidden, t, lambda col: ring[slot, :, col], lambda col: e_step(t, col),
            lambda at, col: c_all[at, col], wt_ref, r_ref, dc_ref, dz, db_ref,
        )

        @pl.when(s + depth < steps)
        def _():
            gates_load(s + depth, slot).start()

        @pl.when(s > 0)
        def _():
            store(s - 1).start()

    store(steps - 1).start()

    @pl.loop(0, steps)
    def _(s):
        store(s).wait()


def backward(layer, e_rows, w_stack, gates, c_all, rows):
    _, _, width = w_stack.shape
    hidden = width // 4
    total = e_rows.shape[0]
    steps = total // rows
    dma = pltpu.SemaphoreType.DMA
    return pl.pallas_call(
        functools.partial(backward_kernel, layer, rows, steps, hidden),
        in_specs=[pl.BlockSpec(memory_space=pl.ANY)] * 4,
        out_specs=[pl.BlockSpec(memory_space=pl.ANY), pl.BlockSpec(memory_space=pltpu.VMEM)],
        out_shape=[
            jax.ShapeDtypeStruct((total, width), jnp.bfloat16),
            jax.ShapeDtypeStruct((8, width), jnp.float32),
        ],
        scratch_shapes=[
            pltpu.VMEM((hidden // 128, total, 128), jnp.float32),
            pltpu.VMEM((hidden, width), jnp.bfloat16),
            pltpu.VMEM((total + rows, hidden), jnp.float32),
            pltpu.VMEM((4, rows, width), jnp.float32),
            pltpu.VMEM((total, width), jnp.bfloat16),
            pltpu.VMEM((width, hidden), jnp.bfloat16),
            pltpu.VMEM((rows, hidden), jnp.float32),
            pltpu.VMEM((rows, hidden), jnp.float32),
            dma((4,)), dma((4,)), dma, dma((hidden // 128 + 1,)),
        ],
        compiler_params=pltpu.CompilerParams(vmem_limit_bytes=VMEM_MAX),
        cost_estimate=pl.CostEstimate(
            flops=20 * 2 * total * hidden * width,
            bytes_accessed=2 * hidden * width + 7 * 4 * total * hidden,
            transcendentals=0,
        ),
        name=f"lstm_backward_{layer}",
    )(e_rows, w_stack, gates, c_all)


MESH = pl.DeviceIdType.MESH
ORDER = (7, 6, 5, 3, 4, 2, 1, 0)
AXES = ((0, 1, 2), (1, 2, 0), (2, 0, 1))


def colour_columns(width):
    tiles = width // 128
    first = -(-tiles // 3)
    second = -(-(tiles - first) // 2)
    sizes = (first * 128, second * 128, (tiles - first - second) * 128)
    return ((0, sizes[0]), (sizes[0], sizes[1]), (sizes[0] + sizes[1], sizes[2]))


def slot_one(code, axes):
    return ((code >> axes[1]) & 1) * 2 + ((code >> axes[2]) & 1)


def add_into(out_ref, a_ref, b_ref):
    @pl.loop(0, out_ref.shape[0] // 16)
    def _(i):
        at = pl.ds(pl.multiple_of(i * 16, 16), 16)
        out_ref[at, :] = a_ref[at, :] + b_ref[at, :]


def grads_kernel(layer, rows, hidden, dz_hbm, db_hbm, x_hbm, h_hbm, w_hbm, gates_hbm, c_hbm, *refs):
    below = layer - 1
    if layer:
        shard_ref, dbsum_ref, dz_out, db_ref, *refs = refs
        dz, uh, uht, w, p, r0, r1, r2, r3, db8, part_db, got_db, *refs = refs
        local_sem, s0, q0, s1, q1, s2, q2, s3, q3, sd, qd, *refs = refs
        dx_ref, c_all, ring, r_ref, dc_ref, ring_sem = refs
    else:
        shard_ref, dbsum_ref, dx_ref, *refs = refs
        dz, uh, uht, w, p, r0, r1, r2, r3, db8, part_db, got_db, *refs = refs
        local_sem, s0, q0, s1, q1, s2, q2, s3, q3, sd, qd = refs
    total, width = dz.shape
    steps = total // rows
    block = 2 * hidden // 16
    parts = width // hidden
    me = lax.axis_index("data")
    z = lax.axis_index("replica")
    y, x, c = me // 4, lax.rem(me // 2, 2), lax.rem(me, 2)
    partner = {"replica": z, "data": y * 4 + x * 2 + 1 - c}
    across = (
        {"replica": z, "data": y * 4 + (1 - x) * 2 + c},
        {"replica": z, "data": (1 - y) * 4 + x * 2 + c},
        {"replica": 1 - z, "data": me},
    )

    u_src = x_hbm if layer == 0 else h_hbm.at[below, pl.ds(rows, total), :]
    loads = [
        pltpu.make_async_copy(u_src, uh.at[:, pl.ds(0, hidden)], local_sem.at[0]),
        pltpu.make_async_copy(h_hbm.at[layer, pl.ds(0, total), :], uh.at[:, pl.ds(hidden, hidden)], local_sem.at[1]),
        pltpu.make_async_copy(dz_hbm, dz, local_sem.at[2]),
        pltpu.make_async_copy(db_hbm, db8, local_sem.at[3]),
        pltpu.make_async_copy(w_hbm.at[layer, pl.ds(0, hidden), :], w, local_sem.at[4]),
    ]
    if layer:
        loads.append(pltpu.make_async_copy(c_hbm.at[below], c_all, local_sem.at[5]))
    for load in loads:
        load.start()

    def gates_load(s, slot):
        at = pl.ds(pl.multiple_of((steps - 1 - s) * rows, rows), rows)
        return pltpu.make_async_copy(gates_hbm.at[below, at, :], ring.at[slot], ring_sem.at[slot])

    depth = 4
    if layer:
        for s in range(min(depth, steps)):
            gates_load(s, s).start()

    barrier = pltpu.get_barrier_semaphore()
    for device in (partner,) + across:
        pl.semaphore_signal(barrier, inc=1, device_id=device, device_id_type=MESH)
    pl.semaphore_wait(barrier, 4)

    def remote(src, dst, send_sem, recv_sem, device):
        return pltpu.make_async_remote_copy(
            src_ref=src, dst_ref=dst, send_sem=send_sem, recv_sem=recv_sem, device_id=device, device_id_type=MESH
        )

    columns = colour_columns(width)
    copies = {}
    for code in range(8):
        for n in range(parts):
            at = code * parts + n
            src = p.at[code, 1 - c, :, pl.ds(n * hidden, hidden)]
            copies[0, code, n] = remote(src, r0.at[pl.ds(at * block, block), :], s0.at[at], q0.at[at], partner)
    for k, axes in enumerate(AXES):
        cols = pl.ds(*columns[k])
        for code in range(8):
            bits = [(code >> axis) & 1 for axis in axes]
            src = p.at[code, c, :, cols]
            if bits[0]:
                slot = slot_one(code, axes)
                at = k * 4 + slot
                copies[1, k, slot] = remote(src, r1.at[slot, :, cols], s1.at[at], q1.at[at], across[axes[0]])
            elif bits[1]:
                at = k * 2 + bits[2]
                copies[2, k, bits[2]] = remote(src, r2.at[bits[2], :, cols], s2.at[at], q2.at[at], across[axes[1]])
            elif bits[2]:
                copies[3, k] = remote(src, r3.at[:, cols], s3.at[k], q3.at[k], across[axes[2]])
    for stage, device in enumerate((partner,) + across):
        copies[4, stage] = remote(part_db.at[stage], got_db.at[stage], sd.at[stage], qd.at[stage], device)

    def bias_stage(stage):
        copies[4, stage].wait_recv()
        out = part_db.at[stage + 1] if stage < 3 else dbsum_ref
        out[...] = part_db[stage] + got_db[stage]
        if stage < 3:
            copies[4, stage + 1].start()

    loads[3].wait()
    part_db[0] = jnp.sum(db8[...], axis=0, keepdims=True).astype(jnp.bfloat16).astype(jnp.float32)
    loads[0].wait()
    loads[1].wait()

    @pl.loop(0, 2 * hidden // 128)
    def _(i):
        at = pl.ds(pl.multiple_of(i * 128, 128), 128)
        uht[at, :] = uh[:, at].T

    copies[4, 0].start()
    loads[2].wait()
    chunk = min(width, 1024)

    def receive_partner(code):
        for n in range(parts):
            copies[0, code, n].wait_recv()
            cols = pl.ds(n * hidden, hidden)
            mine = p.at[code, c, :, cols]
            add_into(mine, mine, r0.at[pl.ds((code * parts + n) * block, block), :])
        for k, axes in enumerate(AXES):
            if (code >> axes[0]) & 1:
                copies[1, k, slot_one(code, axes)].start()

    before = None
    for code in ORDER:
        sides = [
            own + flip - 2 * own * flip
            for own, flip in ((z, (code >> 2) & 1), (y, (code >> 1) & 1), (x, code & 1))
        ]
        base = pl.multiple_of(((sides[0] * 2 + sides[1]) * 2 + sides[2]) * 2 * block, 2 * block)

        @pl.loop(0, width // chunk)
        def _(n):
            cols = pl.ds(pl.multiple_of(n * chunk, chunk), chunk)
            part = jnp.dot(uht[pl.ds(base, 2 * block), :], dz[:, cols], preferred_element_type=jnp.float32)
            low = part.astype(jnp.bfloat16)
            p[code, 0, :, cols] = low[:block]
            p[code, 1, :, cols] = low[block:]

        if before is not None:
            receive_partner(before)
        for n in range(parts):
            copies[0, code, n].start()
        before = code
    receive_partner(before)
    bias_stage(0)

    loads[4].wait()
    step = min(hidden, 512)

    @pl.loop(0, hidden // step)
    def _(n):
        at = pl.ds(pl.multiple_of(n * step, step), step)
        dx_ref[:, at] = lax.dot_general(
            dz[...], w[at, :], (((1,), (1,)), ((), ())), preferred_element_type=jnp.float32
        )

    def first_crossing(codes):
        for code in codes:
            for k, axes in enumerate(AXES):
                if (code >> axes[0]) & 1:
                    slot = slot_one(code, axes)
                    cols = pl.ds(*columns[k])
                    copies[1, k, slot].wait_recv()
                    here = code ^ (1 << axes[0])
                    mine = p.at[here, c, :, cols]
                    add_into(mine, mine, r1.at[slot, :, cols])
                    if (here >> axes[1]) & 1:
                        copies[2, k, (here >> axes[2]) & 1].start()

    def second_crossing(bit):
        for k, axes in enumerate(AXES):
            cols = pl.ds(*columns[k])
            copies[2, k, bit].wait_recv()
            mine = p.at[bit << axes[2], c, :, cols]
            add_into(mine, mine, r2.at[bit, :, cols])
            if bit:
                copies[3, k].start()

    bias_stage(1)
    if layer:
        reload = pltpu.make_async_copy(w_hbm.at[below, pl.ds(hidden, hidden), :], w, local_sem.at[4])
        reload.start()
        r_ref[...] = jnp.zeros_like(r_ref)
        dc_ref[...] = jnp.zeros_like(dc_ref)
        db_ref[...] = jnp.zeros_like(db_ref)
        loads[5].wait()
        reload.wait()
        first_crossing(ORDER[:1])
        for k in range(4):
            transpose_gate(hidden, k, w, r0)

        @pl.loop(0, steps)
        def _(s):
            t = steps - 1 - s
            slot = lax.rem(s, depth)
            gates_load(s, slot).wait()
            now = pl.ds(pl.multiple_of(t * rows, rows), rows)
            backward_step(
                rows, hidden, t, lambda col: ring[slot, :, col], lambda col: dx_ref[now, col],
                lambda at, col: c_all[at, col], r0, r_ref, dc_ref, dz, db_ref,
            )

            @pl.when(s + depth < steps)
            def _():
                gates_load(s + depth, slot).start()

            @pl.when(s == steps // 16)
            def _():
                first_crossing(ORDER[1:4])

            @pl.when(s == steps // 4)
            def _():
                first_crossing(ORDER[4:])

            @pl.when(s == steps // 2)
            def _():
                second_crossing(1)

            @pl.when(s == steps - 3)
            def _():
                second_crossing(0)

        store = pltpu.make_async_copy(dz, dz_out, local_sem.at[2])
        store.start()
    else:
        first_crossing(ORDER)
        second_crossing(1)
        second_crossing(0)
    bias_stage(2)
    bias_stage(3)
    for k in range(3):
        cols = pl.ds(*columns[k])
        copies[3, k].wait_recv()
        add_into(shard_ref.at[:, cols], p.at[0, c, :, cols], r3.at[:, cols])
    for copy in copies.values():
        copy.wait_send()
    if layer:
        store.wait()


def grads(layer, dz, db, x_rows, h_all, w_stack, gates, c_all, rows):
    total, width = dz.shape
    hidden = width // 4
    block = 2 * hidden // 16
    parts = 8 * (width // hidden)
    dma = pltpu.SemaphoreType.DMA
    vmem = pl.BlockSpec(memory_space=pltpu.VMEM)
    hbm = pl.BlockSpec(memory_space=pl.ANY)
    out_shape = [
        jax.ShapeDtypeStruct((block, width), jnp.bfloat16),
        jax.ShapeDtypeStruct((1, width), jnp.float32),
    ]
    scratch = [
        pltpu.VMEM((total, width), jnp.bfloat16),
        pltpu.VMEM((total, 2 * hidden), jnp.bfloat16),
        pltpu.VMEM((2 * hidden, total), jnp.bfloat16),
        pltpu.VMEM((hidden, width), jnp.bfloat16),
        pltpu.VMEM((8, 2, block, width), jnp.bfloat16),
        pltpu.VMEM((width, hidden), jnp.bfloat16),
        pltpu.VMEM((4, block, width), jnp.bfloat16),
        pltpu.VMEM((2, block, width), jnp.bfloat16),
        pltpu.VMEM((block, width), jnp.bfloat16),
        pltpu.VMEM((8, width), jnp.float32),
        pltpu.VMEM((4, 1, width), jnp.float32),
        pltpu.VMEM((4, 1, width), jnp.float32),
        dma((6,)), dma((parts,)), dma((parts,)), dma((12,)), dma((12,)), dma((6,)), dma((6,)), dma((3,)), dma((3,)),
        dma((4,)), dma((4,)),
    ]
    if layer:
        out_specs = [vmem, vmem, hbm, vmem]
        out_shape += [
            jax.ShapeDtypeStruct((total, width), jnp.bfloat16),
            jax.ShapeDtypeStruct((8, width), jnp.float32),
        ]
        scratch += [
            pltpu.VMEM((total, hidden), jnp.float32),
            pltpu.VMEM((total + rows, hidden), jnp.float32),
            pltpu.VMEM((4, rows, width), jnp.float32),
            pltpu.VMEM((rows, hidden), jnp.float32),
            pltpu.VMEM((rows, hidden), jnp.float32),
            dma((4,)),
        ]
    else:
        out_specs = [vmem, vmem, vmem]
        out_shape += [jax.ShapeDtypeStruct((total, hidden), jnp.float32)]
    return pl.pallas_call(
        functools.partial(grads_kernel, layer, rows, hidden),
        in_specs=[hbm] * 7,
        out_specs=out_specs,
        out_shape=out_shape,
        scratch_shapes=scratch,
        compiler_params=pltpu.CompilerParams(
            collective_id=layer, has_side_effects=True, vmem_limit_bytes=VMEM_MAX
        ),
        cost_estimate=pl.CostEstimate(
            flops=6 * total * hidden * width * 5, bytes_accessed=8 * hidden * width, transcendentals=0
        ),
        name=f"lstm_grads_{layer}",
    )(dz, db, x_rows, h_all, w_stack, gates, c_all)


def widen_kernel(part_ref, *refs):
    refs[-1][0] = part_ref[...].astype(jnp.float32)


def widen(total, part, layer, layers):
    height, width = part.shape
    block = min(height, 256)
    return pl.pallas_call(
        widen_kernel,
        grid=(height // block,),
        in_specs=[pl.BlockSpec((block, width), lambda i: (i, 0))]
        + ([] if total is None else [pl.BlockSpec(memory_space=pl.ANY)]),
        out_specs=pl.BlockSpec((1, block, width), lambda i: (layer, i, 0)),
        out_shape=jax.ShapeDtypeStruct((layers, height, width), jnp.float32),
        input_output_aliases={} if total is None else {1: 0},
        cost_estimate=pl.CostEstimate(flops=height * width, bytes_accessed=6 * height * width, transcendentals=0),
        name=f"widen_{layer}",
    )(*([part] if total is None else [part, total]))


def solution(mesh):
    batch_axes = ("replica", "data")

    def local_grads(x_loc, dy_loc, w_stack, b_stack):
        layers, _, width = w_stack.shape
        hidden = width // 4
        rows, steps, _ = x_loc.shape
        x_rows = jnp.swapaxes(x_loc, 0, 1).reshape(steps * rows, hidden)
        e_rows = dy_loc.reshape(rows * steps, hidden)
        h_all, gates, c_all = forward(x_rows, w_stack, b_stack, rows)
        db_list = []
        dw_sum = None
        waiting = None
        dz, db = backward(layers - 1, e_rows, w_stack, gates, c_all, rows)
        for layer in reversed(range(layers)):
            shard, db_sum, *rest = grads(layer, dz, db, x_rows, h_all, w_stack, gates, c_all, rows)
            if layer:
                dz, db = rest
            db_list.append(db_sum)
            if waiting is not None:
                summed, shard = lax.optimization_barrier((waiting, shard))
                dw_sum = widen(dw_sum, summed, layer + 1, layers)
            waiting = lax.all_gather(shard, batch_axes, axis=0, tiled=True)
        e_rows = rest[0]
        db_sum = jnp.concatenate(db_list[::-1], axis=0)
        waiting, dw_sum = lax.optimization_barrier((waiting, dw_sum))
        dw_sum = widen(dw_sum, waiting, 0, layers)
        dx = jnp.swapaxes(e_rows.reshape(steps, rows, hidden), 0, 1)
        return dw_sum, db_sum, dx

    return jax.shard_map(
        local_grads,
        mesh=mesh,
        in_specs=(P(batch_axes), P(batch_axes), P(), P()),
        out_specs=(P(), P(), P(batch_axes)),
        check_vma=False,
    )
```

```python
import functools

import jax
import jax.numpy as jnp
from jax import lax
from jax.experimental import pallas as pl
from jax.experimental.pallas import tpu as pltpu
from jax.sharding import PartitionSpec as P

VMEM_MAX = 67043328
BLK = 256
PAD = 256


def sigmoid(z):
    return 0.5 * jnp.tanh(0.5 * z) + 0.5


def forward_kernel(
    rows, x_hbm, w_hbm, b_ref, h_out, gates_out, c_out,
    h, gates, c, w_in, w_rec, x_sem, first_sem, in_sem, rec_sem, store_sem,
):
    layers, width = b_ref.shape
    hidden = width // 4
    total = gates.shape[1]
    steps = total // rows
    span = total // 4
    group = steps // 4

    def load_in(l, slot):
        return pltpu.make_async_copy(w_hbm.at[l, pl.ds(0, hidden), :], w_in.at[slot, :, pl.ds(0, width)], in_sem.at[slot])

    def load_rec(l, slot):
        return pltpu.make_async_copy(w_hbm.at[l, pl.ds(hidden, hidden), :], w_rec.at[slot, :, pl.ds(0, width)], rec_sem.at[slot])

    def load_first(k):
        cols = pl.ds(k * hidden, hidden)
        return pltpu.make_async_copy(w_hbm.at[0, pl.ds(0, hidden), cols], w_in.at[0, :, cols], first_sem.at[k])

    def stores(l, slot, t):
        now = pl.ds(pl.multiple_of(t * rows, rows), rows)
        later = pl.ds(pl.multiple_of(t * rows + rows, rows), rows)
        return [
            pltpu.make_async_copy(gates.at[slot, now, :], gates_out.at[l, now, :], store_sem.at[slot, 0]),
            pltpu.make_async_copy(h.at[slot, later, :], h_out.at[l, later, :], store_sem.at[slot, 1]),
            pltpu.make_async_copy(c.at[slot, later, :], c_out.at[l, later, :], store_sem.at[slot, 2]),
        ]

    def zero_stores(l, slot):
        at = pl.ds(0, rows)
        return [
            pltpu.make_async_copy(h.at[slot, at, :], h_out.at[l, at, :], store_sem.at[slot, 1]),
            pltpu.make_async_copy(c.at[slot, at, :], c_out.at[l, at, :], store_sem.at[slot, 2]),
        ]

    def finish_stores(l, slot):
        for copy in zero_stores(l, slot):
            copy.wait()

        @pl.loop(0, steps)
        def _(t):
            for copy in stores(l, slot, t):
                copy.wait()

    x_load = pltpu.make_async_copy(x_hbm, h.at[1, pl.ds(rows, total), :], x_sem)
    x_load.start()
    for k in range(4):
        load_first(k).start()
    load_rec(0, 0).start()
    load_in(1, 1).start()
    for slot in range(2):
        h[slot, :rows, :] = jnp.zeros((rows, hidden), jnp.bfloat16)
        c[slot, :rows, :] = jnp.zeros((rows, hidden), jnp.float32)
    x_load.wait()
    for k in range(4):
        load_first(k).wait()

        @pl.loop(0, hidden // BLK)
        def _(n):
            cols = pl.ds(pl.multiple_of(k * hidden + n * BLK, BLK), BLK)
            part = jnp.dot(h[1, rows : rows + 3 * span, :], w_in[0, :, cols], preferred_element_type=jnp.float32)
            gates[0, : 3 * span, cols] = part + b_ref[0:1, cols]

    @pl.loop(0, layers)
    def _(l):
        slot = lax.rem(l, 2)
        other = 1 - slot

        @pl.when(l + 1 < layers)
        def _():
            load_rec(l + 1, other).start()

        for copy in zero_stores(l, slot):
            copy.start()
        load_rec(l, slot).wait()

        @pl.when((l > 0) & (l + 1 < layers))
        def _():
            load_in(l + 1, other).wait()

        @pl.when(l == 0)
        def _():
            load_in(1, 1).wait()

        @pl.loop(0, steps)
        def _(t):
            now = pl.ds(pl.multiple_of(t * rows, rows), rows)
            later = pl.ds(pl.multiple_of(t * rows + rows, rows), rows)
            h_prev = h[slot, now, :]
            for j in range(hidden // BLK):
                cols = [pl.ds(k * hidden + j * BLK, BLK) for k in range(4)]
                z = [
                    gates[slot, now, col]
                    + jnp.dot(h_prev, w_rec[slot, :, col], preferred_element_type=jnp.float32)
                    for col in cols
                ]
                if j == hidden // BLK - 1:
                    early = t < group
                    source = jnp.where(early, other, slot)
                    target = jnp.where(early, slot, other)
                    row = pl.multiple_of(jnp.where(early, 3, t // group - 1) * span, span)
                    bias = jnp.minimum(jnp.where(early, l, l + 1), layers - 1)
                    u = h[source, pl.ds(pl.multiple_of(row + rows, rows), span), :]
                    for i in range(width // group // BLK):
                        col = pl.ds(pl.multiple_of(lax.rem(t, group) * (width // group) + i * BLK, BLK), BLK)
                        gates[target, pl.ds(row, span), col] = b_ref[pl.ds(bias, 1), col] + jnp.dot(
                            u, w_in[target, :, col], preferred_element_type=jnp.float32
                        )
                act = [sigmoid(z[0]), sigmoid(z[1]), jnp.tanh(z[2]), sigmoid(z[3])]
                for col, value in zip(cols, act):
                    gates[slot, now, col] = value
                part = pl.ds(j * BLK, BLK)
                c_new = act[1] * c[slot, now, part] + act[0] * act[2]
                c[slot, later, part] = c_new
                h[slot, later, part] = (act[3] * jnp.tanh(c_new)).astype(jnp.bfloat16)

            @pl.when(t > 0)
            def _():
                for copy in stores(l, slot, t - 1):
                    copy.start()

            @pl.when(t == group - 1)
            def _():
                @pl.when(l > 0)
                def _():
                    finish_stores(l - 1, other)

                @pl.when(l + 2 < layers)
                def _():
                    load_in(l + 2, slot).start()

        for copy in stores(l, slot, steps - 1):
            copy.start()

    finish_stores(layers - 1, (layers - 1) % 2)


def forward(x_rows, w_stack, b_stack, rows):
    layers, _, width = w_stack.shape
    hidden = width // 4
    total = x_rows.shape[0]
    dma = pltpu.SemaphoreType.DMA
    hbm = pl.BlockSpec(memory_space=pl.ANY)
    return pl.pallas_call(
        functools.partial(forward_kernel, rows),
        in_specs=[hbm, hbm, pl.BlockSpec(memory_space=pltpu.VMEM)],
        out_specs=[hbm] * 3,
        out_shape=[
            jax.ShapeDtypeStruct((layers, total + rows, hidden), jnp.bfloat16),
            jax.ShapeDtypeStruct((layers, total, width), jnp.float32),
            jax.ShapeDtypeStruct((layers, total + rows, hidden), jnp.float32),
        ],
        scratch_shapes=[
            pltpu.VMEM((2, total + rows, hidden), jnp.bfloat16),
            pltpu.VMEM((2, total, width), jnp.float32),
            pltpu.VMEM((2, total + rows, hidden), jnp.float32),
            pltpu.VMEM((2, hidden, width + PAD), jnp.bfloat16),
            pltpu.VMEM((2, hidden, width + PAD), jnp.bfloat16),
            dma, dma((4,)), dma((2,)), dma((2,)), dma((2, 3)),
        ],
        compiler_params=pltpu.CompilerParams(vmem_limit_bytes=VMEM_MAX),
        cost_estimate=pl.CostEstimate(
            flops=2 * layers * total * 2 * hidden * width,
            bytes_accessed=2 * layers * hidden * width + 5 * 4 * layers * total * hidden,
            transcendentals=0,
        ),
        name="lstm_forward",
    )(x_rows, w_stack, b_stack)


def backward_step(rows, hidden, t, gate, e, c, wt_ref, r_ref, dc_ref, dz_ref, db_ref):
    now = pl.ds(pl.multiple_of(t * rows, rows), rows)
    later = pl.ds(pl.multiple_of(t * rows + rows, rows), rows)
    total = None
    for j in range(hidden // BLK):
        part = pl.ds(j * BLK, BLK)
        cols = [pl.ds(k * hidden + j * BLK, BLK) for k in range(4)]
        gate_i, gate_f, gate_g, gate_o = [gate(col) for col in cols]
        tanh_c = jnp.tanh(c(later, part))
        dh = e(part) + r_ref[:, part]
        dc = dc_ref[:, part] + dh * gate_o * (1.0 - tanh_c * tanh_c)
        dz = [
            dc * gate_g * gate_i * (1.0 - gate_i),
            dc * c(now, part) * gate_f * (1.0 - gate_f),
            dc * gate_i * (1.0 - gate_g * gate_g),
            dh * tanh_c * gate_o * (1.0 - gate_o),
        ]
        dc_ref[:, part] = dc * gate_f
        low = []
        for col, value in zip(cols, dz):
            low.append(value.astype(jnp.bfloat16))
            dz_ref[now, col] = low[-1]
            db_ref[:, col] += jnp.sum(value.reshape(rows // 8, 8, BLK), axis=0)
        back = jnp.dot(
            jnp.concatenate(low, axis=1),
            wt_ref[j * 4 * BLK : (j + 1) * 4 * BLK, :hidden],
            preferred_element_type=jnp.float32,
        )
        total = back if total is None else total + back
    r_ref[...] = total


def transpose_gate(hidden, k, w_ref, wt_ref):
    @pl.loop(0, hidden // BLK)
    def _(j):
        cols = pl.ds(pl.multiple_of(k * hidden + j * BLK, BLK), BLK)
        place = pl.ds(pl.multiple_of(j * 4 * BLK + k * BLK, BLK), BLK)
        wt_ref[place, :hidden] = w_ref[:, cols].T


def backward_kernel(
    layer, rows, steps, hidden, e_hbm, w_hbm, gates_hbm, c_hbm, dz_out, db_ref,
    e_all, w, c_all, ring, dz, wt_ref, r_ref, dc_ref, w_sem, ring_sem, out_sem, sem,
):
    depth = ring.shape[0]

    def gates_load(s, slot):
        at = pl.ds(pl.multiple_of((steps - 1 - s) * rows, rows), rows)
        return pltpu.make_async_copy(gates_hbm.at[layer, at, :], ring.at[slot], ring_sem.at[slot])

    def store(s):
        at = pl.ds(pl.multiple_of((steps - 1 - s) * rows, rows), rows)
        return pltpu.make_async_copy(dz.at[at, :], dz_out.at[at, :], out_sem)

    def e_step(t, col):
        first, count = col.start // 128, col.size // 128
        at = pl.ds(t, rows, stride=steps)
        return jnp.concatenate([e_all[first + i, at, :] for i in range(count)], axis=1)

    def w_load(k):
        cols = pl.ds(k * hidden, hidden)
        return pltpu.make_async_copy(w_hbm.at[layer, pl.ds(hidden, hidden), cols], w.at[:, cols], w_sem.at[k])

    tiles = hidden // 128
    loads = [pltpu.make_async_copy(c_hbm.at[layer], c_all, sem.at[tiles])]
    for i in range(tiles):
        loads.append(pltpu.make_async_copy(e_hbm.at[:, pl.ds(i * 128, 128)], e_all.at[i], sem.at[i]))
    for k in range(4):
        w_load(k).start()
    for load in loads:
        load.start()
    for s in range(min(depth, steps)):
        gates_load(s, s).start()
    r_ref[...] = jnp.zeros_like(r_ref)
    dc_ref[...] = jnp.zeros_like(dc_ref)
    db_ref[...] = jnp.zeros_like(db_ref)
    for k in range(4):
        w_load(k).wait()
        transpose_gate(hidden, k, w, wt_ref)
    for load in loads:
        load.wait()

    @pl.loop(0, steps)
    def _(s):
        t = steps - 1 - s
        slot = lax.rem(s, depth)
        gates_load(s, slot).wait()
        backward_step(
            rows, hidden, t, lambda col: ring[slot, :, col], lambda col: e_step(t, col),
            lambda at, col: c_all[at, col], wt_ref, r_ref, dc_ref, dz, db_ref,
        )

        @pl.when(s + depth < steps)
        def _():
            gates_load(s + depth, slot).start()

        @pl.when(s > 0)
        def _():
            store(s - 1).start()

    store(steps - 1).start()

    @pl.loop(0, steps)
    def _(s):
        store(s).wait()


def backward(layer, e_rows, w_stack, gates, c_all, rows):
    _, _, width = w_stack.shape
    hidden = width // 4
    total = e_rows.shape[0]
    steps = total // rows
    dma = pltpu.SemaphoreType.DMA
    return pl.pallas_call(
        functools.partial(backward_kernel, layer, rows, steps, hidden),
        in_specs=[pl.BlockSpec(memory_space=pl.ANY)] * 4,
        out_specs=[pl.BlockSpec(memory_space=pl.ANY), pl.BlockSpec(memory_space=pltpu.VMEM)],
        out_shape=[
            jax.ShapeDtypeStruct((total, width), jnp.bfloat16),
            jax.ShapeDtypeStruct((8, width), jnp.float32),
        ],
        scratch_shapes=[
            pltpu.VMEM((hidden // 128, total, 128), jnp.float32),
            pltpu.VMEM((hidden, width), jnp.bfloat16),
            pltpu.VMEM((total + rows, hidden), jnp.float32),
            pltpu.VMEM((4, rows, width), jnp.float32),
            pltpu.VMEM((total, width), jnp.bfloat16),
            pltpu.VMEM((width, hidden + PAD), jnp.bfloat16),
            pltpu.VMEM((rows, hidden), jnp.float32),
            pltpu.VMEM((rows, hidden), jnp.float32),
            dma((4,)), dma((4,)), dma, dma((hidden // 128 + 1,)),
        ],
        compiler_params=pltpu.CompilerParams(vmem_limit_bytes=VMEM_MAX),
        cost_estimate=pl.CostEstimate(
            flops=20 * 2 * total * hidden * width,
            bytes_accessed=2 * hidden * width + 7 * 4 * total * hidden,
            transcendentals=0,
        ),
        name=f"lstm_backward_{layer}",
    )(e_rows, w_stack, gates, c_all)


MESH = pl.DeviceIdType.MESH
ORDER = (7, 6, 5, 3, 4, 2, 1, 0)
AXES = ((0, 1, 2), (1, 2, 0), (2, 0, 1))


def colour_columns(width):
    tiles = width // 128
    first = -(-tiles // 3)
    second = -(-(tiles - first) // 2)
    sizes = (first * 128, second * 128, (tiles - first - second) * 128)
    return ((0, sizes[0]), (sizes[0], sizes[1]), (sizes[0] + sizes[1], sizes[2]))


def slot_one(code, axes):
    return ((code >> axes[1]) & 1) * 2 + ((code >> axes[2]) & 1)


def add_into(out_ref, a_ref, b_ref):
    @pl.loop(0, out_ref.shape[0] // 16)
    def _(i):
        at = pl.ds(pl.multiple_of(i * 16, 16), 16)
        out_ref[at, :] = a_ref[at, :] + b_ref[at, :]


def grads_kernel(layer, rows, hidden, dz_hbm, db_hbm, x_hbm, h_hbm, w_hbm, gates_hbm, c_hbm, *refs):
    below = layer - 1
    if layer:
        shard_ref, dbsum_ref, dz_out, db_ref, *refs = refs
        dz, uh, uht, w, p, r0, r1, r2, r3, db8, part_db, got_db, *refs = refs
        local_sem, s0, q0, s1, q1, s2, q2, s3, q3, sd, qd, *refs = refs
        dx_ref, c_all, ring, r_ref, dc_ref, ring_sem = refs
    else:
        shard_ref, dbsum_ref, dx_ref, *refs = refs
        dz, uh, uht, w, p, r0, r1, r2, r3, db8, part_db, got_db, *refs = refs
        local_sem, s0, q0, s1, q1, s2, q2, s3, q3, sd, qd = refs
    total, width = dz.shape
    steps = total // rows
    block = 2 * hidden // 16
    parts = width // hidden
    me = lax.axis_index("data")
    z = lax.axis_index("replica")
    y, x, c = me // 4, lax.rem(me // 2, 2), lax.rem(me, 2)
    partner = {"replica": z, "data": y * 4 + x * 2 + 1 - c}
    across = (
        {"replica": z, "data": y * 4 + (1 - x) * 2 + c},
        {"replica": z, "data": (1 - y) * 4 + x * 2 + c},
        {"replica": 1 - z, "data": me},
    )

    u_src = x_hbm if layer == 0 else h_hbm.at[below, pl.ds(rows, total), :]
    loads = [
        pltpu.make_async_copy(u_src, uh.at[:, pl.ds(0, hidden)], local_sem.at[0]),
        pltpu.make_async_copy(h_hbm.at[layer, pl.ds(0, total), :], uh.at[:, pl.ds(hidden, hidden)], local_sem.at[1]),
        pltpu.make_async_copy(dz_hbm, dz, local_sem.at[2]),
        pltpu.make_async_copy(db_hbm, db8, local_sem.at[3]),
        pltpu.make_async_copy(w_hbm.at[layer, pl.ds(0, hidden), :], w, local_sem.at[4]),
    ]
    if layer:
        loads.append(pltpu.make_async_copy(c_hbm.at[below], c_all, local_sem.at[5]))
    for load in loads:
        load.start()

    def gates_load(s, slot):
        at = pl.ds(pl.multiple_of((steps - 1 - s) * rows, rows), rows)
        return pltpu.make_async_copy(gates_hbm.at[below, at, :], ring.at[slot], ring_sem.at[slot])

    depth = 4
    if layer:
        for s in range(min(depth, steps)):
            gates_load(s, s).start()

    barrier = pltpu.get_barrier_semaphore()
    for device in (partner,) + across:
        pl.semaphore_signal(barrier, inc=1, device_id=device, device_id_type=MESH)
    pl.semaphore_wait(barrier, 4)

    def remote(src, dst, send_sem, recv_sem, device):
        return pltpu.make_async_remote_copy(
            src_ref=src, dst_ref=dst, send_sem=send_sem, recv_sem=recv_sem, device_id=device, device_id_type=MESH
        )

    columns = colour_columns(width)
    copies = {}
    for code in range(8):
        for n in range(parts):
            at = code * parts + n
            src = p.at[code, 1 - c, :, pl.ds(n * hidden, hidden)]
            copies[0, code, n] = remote(src, r0.at[pl.ds(at * block, block), pl.ds(0, hidden)], s0.at[at], q0.at[at], partner)
    for k, axes in enumerate(AXES):
        cols = pl.ds(*columns[k])
        for code in range(8):
            bits = [(code >> axis) & 1 for axis in axes]
            src = p.at[code, c, :, cols]
            if bits[0]:
                slot = slot_one(code, axes)
                at = k * 4 + slot
                copies[1, k, slot] = remote(src, r1.at[slot, :, cols], s1.at[at], q1.at[at], across[axes[0]])
            elif bits[1]:
                at = k * 2 + bits[2]
                copies[2, k, bits[2]] = remote(src, r2.at[bits[2], :, cols], s2.at[at], q2.at[at], across[axes[1]])
            elif bits[2]:
                copies[3, k] = remote(src, r3.at[:, cols], s3.at[k], q3.at[k], across[axes[2]])
    for stage, device in enumerate((partner,) + across):
        copies[4, stage] = remote(part_db.at[stage], got_db.at[stage], sd.at[stage], qd.at[stage], device)

    def bias_stage(stage):
        copies[4, stage].wait_recv()
        out = part_db.at[stage + 1] if stage < 3 else dbsum_ref
        out[...] = part_db[stage] + got_db[stage]
        if stage < 3:
            copies[4, stage + 1].start()

    loads[3].wait()
    part_db[0] = jnp.sum(db8[...], axis=0, keepdims=True).astype(jnp.bfloat16).astype(jnp.float32)
    loads[0].wait()
    loads[1].wait()

    @pl.loop(0, 2 * hidden // 128)
    def _(i):
        at = pl.ds(pl.multiple_of(i * 128, 128), 128)
        uht[at, :] = uh[:, at].T

    copies[4, 0].start()
    loads[2].wait()
    chunk = min(width, 1024)

    def receive_partner(code):
        for n in range(parts):
            copies[0, code, n].wait_recv()
            cols = pl.ds(n * hidden, hidden)
            mine = p.at[code, c, :, cols]
            add_into(mine, mine, r0.at[pl.ds((code * parts + n) * block, block), pl.ds(0, hidden)])
        for k, axes in enumerate(AXES):
            if (code >> axes[0]) & 1:
                copies[1, k, slot_one(code, axes)].start()

    before = None
    for code in ORDER:
        sides = [
            own + flip - 2 * own * flip
            for own, flip in ((z, (code >> 2) & 1), (y, (code >> 1) & 1), (x, code & 1))
        ]
        base = pl.multiple_of(((sides[0] * 2 + sides[1]) * 2 + sides[2]) * 2 * block, 2 * block)

        @pl.loop(0, width // chunk)
        def _(n):
            cols = pl.ds(pl.multiple_of(n * chunk, chunk), chunk)
            part = jnp.dot(uht[pl.ds(base, 2 * block), :], dz[:, cols], preferred_element_type=jnp.float32)
            low = part.astype(jnp.bfloat16)
            p[code, 0, :, cols] = low[:block]
            p[code, 1, :, cols] = low[block:]

        if before is not None:
            receive_partner(before)
        for n in range(parts):
            copies[0, code, n].start()
        before = code
    receive_partner(before)
    bias_stage(0)

    loads[4].wait()
    step = BLK

    @pl.loop(0, hidden // step)
    def _(n):
        at = pl.ds(pl.multiple_of(n * step, step), step)
        dx_ref[:, at] = lax.dot_general(
            dz[...], w[at, :], (((1,), (1,)), ((), ())), preferred_element_type=jnp.float32
        )

    def first_crossing(codes):
        for code in codes:
            for k, axes in enumerate(AXES):
                if (code >> axes[0]) & 1:
                    slot = slot_one(code, axes)
                    cols = pl.ds(*columns[k])
                    copies[1, k, slot].wait_recv()
                    here = code ^ (1 << axes[0])
                    mine = p.at[here, c, :, cols]
                    add_into(mine, mine, r1.at[slot, :, cols])
                    if (here >> axes[1]) & 1:
                        copies[2, k, (here >> axes[2]) & 1].start()

    def second_crossing(bit):
        for k, axes in enumerate(AXES):
            cols = pl.ds(*columns[k])
            copies[2, k, bit].wait_recv()
            mine = p.at[bit << axes[2], c, :, cols]
            add_into(mine, mine, r2.at[bit, :, cols])
            if bit:
                copies[3, k].start()

    bias_stage(1)
    if layer:
        reload = pltpu.make_async_copy(w_hbm.at[below, pl.ds(hidden, hidden), :], w, local_sem.at[4])
        reload.start()
        r_ref[...] = jnp.zeros_like(r_ref)
        dc_ref[...] = jnp.zeros_like(dc_ref)
        db_ref[...] = jnp.zeros_like(db_ref)
        loads[5].wait()
        reload.wait()
        first_crossing(ORDER[:1])
        for k in range(4):
            transpose_gate(hidden, k, w, r0)

        @pl.loop(0, steps)
        def _(s):
            t = steps - 1 - s
            slot = lax.rem(s, depth)
            gates_load(s, slot).wait()
            now = pl.ds(pl.multiple_of(t * rows, rows), rows)
            backward_step(
                rows, hidden, t, lambda col: ring[slot, :, col], lambda col: dx_ref[now, col],
                lambda at, col: c_all[at, col], r0, r_ref, dc_ref, dz, db_ref,
            )

            @pl.when(s + depth < steps)
            def _():
                gates_load(s + depth, slot).start()

            @pl.when(s == steps // 16)
            def _():
                first_crossing(ORDER[1:4])

            @pl.when(s == steps // 4)
            def _():
                first_crossing(ORDER[4:])

            @pl.when(s == steps // 2)
            def _():
                second_crossing(1)

            @pl.when(s == steps - 3)
            def _():
                second_crossing(0)

        store = pltpu.make_async_copy(dz, dz_out, local_sem.at[2])
        store.start()
    else:
        first_crossing(ORDER)
        second_crossing(1)
        second_crossing(0)
    bias_stage(2)
    bias_stage(3)
    for k in range(3):
        cols = pl.ds(*columns[k])
        copies[3, k].wait_recv()
        add_into(shard_ref.at[:, cols], p.at[0, c, :, cols], r3.at[:, cols])
    for copy in copies.values():
        copy.wait_send()
    if layer:
        store.wait()


def grads(layer, dz, db, x_rows, h_all, w_stack, gates, c_all, rows):
    total, width = dz.shape
    hidden = width // 4
    block = 2 * hidden // 16
    parts = 8 * (width // hidden)
    dma = pltpu.SemaphoreType.DMA
    vmem = pl.BlockSpec(memory_space=pltpu.VMEM)
    hbm = pl.BlockSpec(memory_space=pl.ANY)
    out_shape = [
        jax.ShapeDtypeStruct((block, width), jnp.bfloat16),
        jax.ShapeDtypeStruct((1, width), jnp.float32),
    ]
    scratch = [
        pltpu.VMEM((total, width), jnp.bfloat16),
        pltpu.VMEM((total, 2 * hidden), jnp.bfloat16),
        pltpu.VMEM((2 * hidden, total), jnp.bfloat16),
        pltpu.VMEM((hidden, width), jnp.bfloat16),
        pltpu.VMEM((8, 2, block, width), jnp.bfloat16),
        pltpu.VMEM((width, hidden + PAD), jnp.bfloat16),
        pltpu.VMEM((4, block, width), jnp.bfloat16),
        pltpu.VMEM((2, block, width), jnp.bfloat16),
        pltpu.VMEM((block, width), jnp.bfloat16),
        pltpu.VMEM((8, width), jnp.float32),
        pltpu.VMEM((4, 1, width), jnp.float32),
        pltpu.VMEM((4, 1, width), jnp.float32),
        dma((6,)), dma((parts,)), dma((parts,)), dma((12,)), dma((12,)), dma((6,)), dma((6,)), dma((3,)), dma((3,)),
        dma((4,)), dma((4,)),
    ]
    if layer:
        out_specs = [vmem, vmem, hbm, vmem]
        out_shape += [
            jax.ShapeDtypeStruct((total, width), jnp.bfloat16),
            jax.ShapeDtypeStruct((8, width), jnp.float32),
        ]
        scratch += [
            pltpu.VMEM((total, hidden), jnp.float32),
            pltpu.VMEM((total + rows, hidden), jnp.float32),
            pltpu.VMEM((4, rows, width), jnp.float32),
            pltpu.VMEM((rows, hidden), jnp.float32),
            pltpu.VMEM((rows, hidden), jnp.float32),
            dma((4,)),
        ]
    else:
        out_specs = [vmem, vmem, vmem]
        out_shape += [jax.ShapeDtypeStruct((total, hidden), jnp.float32)]
    return pl.pallas_call(
        functools.partial(grads_kernel, layer, rows, hidden),
        in_specs=[hbm] * 7,
        out_specs=out_specs,
        out_shape=out_shape,
        scratch_shapes=scratch,
        compiler_params=pltpu.CompilerParams(
            collective_id=layer, has_side_effects=True, vmem_limit_bytes=VMEM_MAX
        ),
        cost_estimate=pl.CostEstimate(
            flops=6 * total * hidden * width * 5, bytes_accessed=8 * hidden * width, transcendentals=0
        ),
        name=f"lstm_grads_{layer}",
    )(dz, db, x_rows, h_all, w_stack, gates, c_all)


def widen_kernel(part_ref, *refs):
    refs[-1][0] = part_ref[...].astype(jnp.float32)


def widen(total, part, layer, layers):
    height, width = part.shape
    block = min(height, 128)
    return pl.pallas_call(
        widen_kernel,
        grid=(height // block,),
        in_specs=[pl.BlockSpec((block, width), lambda i: (i, 0))]
        + ([] if total is None else [pl.BlockSpec(memory_space=pl.ANY)]),
        out_specs=pl.BlockSpec((1, block, width), lambda i: (layer, i, 0)),
        out_shape=jax.ShapeDtypeStruct((layers, height, width), jnp.float32),
        input_output_aliases={} if total is None else {1: 0},
        cost_estimate=pl.CostEstimate(flops=height * width, bytes_accessed=6 * height * width, transcendentals=0),
        name=f"widen_{layer}",
    )(*([part] if total is None else [part, total]))


def solution(mesh):
    batch_axes = ("replica", "data")

    def local_grads(x_loc, dy_loc, w_stack, b_stack):
        layers, _, width = w_stack.shape
        hidden = width // 4
        rows, steps, _ = x_loc.shape
        x_rows = jnp.swapaxes(x_loc, 0, 1).reshape(steps * rows, hidden)
        e_rows = dy_loc.reshape(rows * steps, hidden)
        h_all, gates, c_all = forward(x_rows, w_stack, b_stack, rows)
        db_list = []
        dw_sum = None
        waiting = None
        dz, db = backward(layers - 1, e_rows, w_stack, gates, c_all, rows)
        for layer in reversed(range(layers)):
            shard, db_sum, *rest = grads(layer, dz, db, x_rows, h_all, w_stack, gates, c_all, rows)
            if layer:
                dz, db = rest
            db_list.append(db_sum)
            if waiting is not None:
                summed, shard = lax.optimization_barrier((waiting, shard))
                dw_sum = widen(dw_sum, summed, layer + 1, layers)
            waiting = lax.all_gather(shard, batch_axes, axis=0, tiled=True)
        e_rows = rest[0]
        db_sum = jnp.concatenate(db_list[::-1], axis=0)
        waiting, dw_sum = lax.optimization_barrier((waiting, dw_sum))
        dw_sum = widen(dw_sum, waiting, 0, layers)
        dx = jnp.swapaxes(e_rows.reshape(steps, rows, hidden), 0, 1)
        return dw_sum, db_sum, dx

    return jax.shard_map(
        local_grads,
        mesh=mesh,
        in_specs=(P(batch_axes), P(batch_axes), P(), P()),
        out_specs=(P(), P(), P(batch_axes)),
        check_vma=False,
    )
```

```python
import functools

import jax
import jax.numpy as jnp
from jax import lax
from jax.experimental import pallas as pl
from jax.experimental.pallas import tpu as pltpu
from jax.sharding import PartitionSpec as P

VMEM_MAX = 67043328
BLK = 256
PAD = 256


def sigmoid(z):
    return 0.5 * jnp.tanh(0.5 * z) + 0.5


def forward_kernel(
    rows, x_hbm, w_hbm, b_ref, h_out, gates_out, c_out,
    h, gates, c, w_in, w_rec, x_sem, first_sem, in_sem, rec_sem, store_sem,
):
    layers, width = b_ref.shape
    hidden = width // 4
    total = gates.shape[1]
    steps = total // rows
    span = total // 4
    group = steps // 4

    def load_in(l, slot):
        return pltpu.make_async_copy(w_hbm.at[l, pl.ds(0, hidden), :], w_in.at[slot, :, pl.ds(0, width)], in_sem.at[slot])

    def load_rec(l, slot):
        return pltpu.make_async_copy(w_hbm.at[l, pl.ds(hidden, hidden), :], w_rec.at[slot, :, pl.ds(0, width)], rec_sem.at[slot])

    def load_first(k):
        cols = pl.ds(k * hidden, hidden)
        return pltpu.make_async_copy(w_hbm.at[0, pl.ds(0, hidden), cols], w_in.at[0, :, cols], first_sem.at[k])

    def stores(l, slot, t):
        now = pl.ds(pl.multiple_of(t * rows, rows), rows)
        later = pl.ds(pl.multiple_of(t * rows + rows, rows), rows)
        return [
            pltpu.make_async_copy(gates.at[slot, now, :], gates_out.at[l, now, :], store_sem.at[slot, 0]),
            pltpu.make_async_copy(h.at[slot, later, :], h_out.at[l, later, :], store_sem.at[slot, 1]),
            pltpu.make_async_copy(c.at[slot, later, :], c_out.at[l, later, :], store_sem.at[slot, 2]),
        ]

    def zero_stores(l, slot):
        at = pl.ds(0, rows)
        return [
            pltpu.make_async_copy(h.at[slot, at, :], h_out.at[l, at, :], store_sem.at[slot, 1]),
            pltpu.make_async_copy(c.at[slot, at, :], c_out.at[l, at, :], store_sem.at[slot, 2]),
        ]

    def finish_stores(l, slot):
        for copy in zero_stores(l, slot):
            copy.wait()

        @pl.loop(0, steps)
        def _(t):
            for copy in stores(l, slot, t):
                copy.wait()

    x_load = pltpu.make_async_copy(x_hbm, h.at[1, pl.ds(rows, total), :], x_sem)
    x_load.start()
    for k in range(4):
        load_first(k).start()
    load_rec(0, 0).start()
    load_in(1, 1).start()
    for slot in range(2):
        h[slot, :rows, :] = jnp.zeros((rows, hidden), jnp.bfloat16)
        c[slot, :rows, :] = jnp.zeros((rows, hidden), jnp.float32)
    x_load.wait()
    for k in range(4):
        load_first(k).wait()

        @pl.loop(0, hidden // BLK)
        def _(n):
            cols = pl.ds(pl.multiple_of(k * hidden + n * BLK, BLK), BLK)
            part = jnp.dot(h[1, rows : rows + 3 * span, :], w_in[0, :, cols], preferred_element_type=jnp.float32)
            gates[0, : 3 * span, cols] = part + b_ref[0:1, cols]

    @pl.loop(0, layers)
    def _(l):
        slot = lax.rem(l, 2)
        other = 1 - slot

        @pl.when(l + 1 < layers)
        def _():
            load_rec(l + 1, other).start()

        for copy in zero_stores(l, slot):
            copy.start()
        load_rec(l, slot).wait()

        @pl.when((l > 0) & (l + 1 < layers))
        def _():
            load_in(l + 1, other).wait()

        @pl.when(l == 0)
        def _():
            load_in(1, 1).wait()

        @pl.loop(0, steps)
        def _(t):
            now = pl.ds(pl.multiple_of(t * rows, rows), rows)
            later = pl.ds(pl.multiple_of(t * rows + rows, rows), rows)
            h_prev = h[slot, now, :]
            for j in range(hidden // BLK):
                cols = [pl.ds(k * hidden + j * BLK, BLK) for k in range(4)]
                z = [
                    gates[slot, now, col]
                    + jnp.dot(h_prev, w_rec[slot, :, col], preferred_element_type=jnp.float32)
                    for col in cols
                ]
                if j == hidden // BLK - 1:
                    early = t < group
                    source = jnp.where(early, other, slot)
                    target = jnp.where(early, slot, other)
                    row = pl.multiple_of(jnp.where(early, 3, t // group - 1) * span, span)
                    bias = jnp.minimum(jnp.where(early, l, l + 1), layers - 1)
                    u = h[source, pl.ds(pl.multiple_of(row + rows, rows), span), :]
                    for i in range(width // group // BLK):
                        col = pl.ds(pl.multiple_of(lax.rem(t, group) * (width // group) + i * BLK, BLK), BLK)
                        gates[target, pl.ds(row, span), col] = b_ref[pl.ds(bias, 1), col] + jnp.dot(
                            u, w_in[target, :, col], preferred_element_type=jnp.float32
                        )
                act = [sigmoid(z[0]), sigmoid(z[1]), jnp.tanh(z[2]), sigmoid(z[3])]
                for col, value in zip(cols, act):
                    gates[slot, now, col] = value
                part = pl.ds(j * BLK, BLK)
                c_new = act[1] * c[slot, now, part] + act[0] * act[2]
                c[slot, later, part] = c_new
                h[slot, later, part] = (act[3] * jnp.tanh(c_new)).astype(jnp.bfloat16)

            @pl.when(t > 0)
            def _():
                for copy in stores(l, slot, t - 1):
                    copy.start()

            @pl.when(t == group - 1)
            def _():
                @pl.when(l > 0)
                def _():
                    finish_stores(l - 1, other)

                @pl.when(l + 2 < layers)
                def _():
                    load_in(l + 2, slot).start()

        for copy in stores(l, slot, steps - 1):
            copy.start()

    finish_stores(layers - 1, (layers - 1) % 2)


def forward(x_rows, w_stack, b_stack, rows):
    layers, _, width = w_stack.shape
    hidden = width // 4
    total = x_rows.shape[0]
    dma = pltpu.SemaphoreType.DMA
    hbm = pl.BlockSpec(memory_space=pl.ANY)
    return pl.pallas_call(
        functools.partial(forward_kernel, rows),
        in_specs=[hbm, hbm, pl.BlockSpec(memory_space=pltpu.VMEM)],
        out_specs=[hbm] * 3,
        out_shape=[
            jax.ShapeDtypeStruct((layers, total + rows, hidden), jnp.bfloat16),
            jax.ShapeDtypeStruct((layers, total, width), jnp.float32),
            jax.ShapeDtypeStruct((layers, total + rows, hidden), jnp.float32),
        ],
        scratch_shapes=[
            pltpu.VMEM((2, total + rows, hidden), jnp.bfloat16),
            pltpu.VMEM((2, total, width), jnp.float32),
            pltpu.VMEM((2, total + rows, hidden), jnp.float32),
            pltpu.VMEM((2, hidden, width + PAD), jnp.bfloat16),
            pltpu.VMEM((2, hidden, width + PAD), jnp.bfloat16),
            dma, dma((4,)), dma((2,)), dma((2,)), dma((2, 3)),
        ],
        compiler_params=pltpu.CompilerParams(vmem_limit_bytes=VMEM_MAX),
        cost_estimate=pl.CostEstimate(
            flops=2 * layers * total * 2 * hidden * width,
            bytes_accessed=2 * layers * hidden * width + 5 * 4 * layers * total * hidden,
            transcendentals=0,
        ),
        name="lstm_forward",
    )(x_rows, w_stack, b_stack)


def backward_step(rows, hidden, t, gate, e, c, wt_ref, r_ref, dc_ref, dz_ref, db_ref):
    now = pl.ds(pl.multiple_of(t * rows, rows), rows)
    later = pl.ds(pl.multiple_of(t * rows + rows, rows), rows)
    total = None
    for j in range(hidden // BLK):
        part = pl.ds(j * BLK, BLK)
        cols = [pl.ds(k * hidden + j * BLK, BLK) for k in range(4)]
        gate_i, gate_f, gate_g, gate_o = [gate(col) for col in cols]
        tanh_c = jnp.tanh(c(later, part))
        dh = e(part) + r_ref[:, part]
        dc = dc_ref[:, part] + dh * gate_o * (1.0 - tanh_c * tanh_c)
        dz = [
            dc * gate_g * gate_i * (1.0 - gate_i),
            dc * c(now, part) * gate_f * (1.0 - gate_f),
            dc * gate_i * (1.0 - gate_g * gate_g),
            dh * tanh_c * gate_o * (1.0 - gate_o),
        ]
        dc_ref[:, part] = dc * gate_f
        low = []
        for col, value in zip(cols, dz):
            low.append(value.astype(jnp.bfloat16))
            dz_ref[now, col] = low[-1]
            db_ref[:, col] += jnp.sum(value.reshape(rows // 8, 8, BLK), axis=0)
        back = jnp.dot(
            jnp.concatenate(low, axis=1),
            wt_ref[j * 4 * BLK : (j + 1) * 4 * BLK, :hidden],
            preferred_element_type=jnp.float32,
        )
        total = back if total is None else total + back
    r_ref[...] = total


def transpose_gate(hidden, k, w_ref, wt_ref):
    @pl.loop(0, hidden // BLK)
    def _(j):
        cols = pl.ds(pl.multiple_of(k * hidden + j * BLK, BLK), BLK)
        place = pl.ds(pl.multiple_of(j * 4 * BLK + k * BLK, BLK), BLK)
        wt_ref[place, :hidden] = w_ref[:, cols].T


def backward_kernel(
    layer, rows, steps, hidden, e_hbm, w_hbm, gates_hbm, c_hbm, dz_out, db_ref,
    e_all, w, c_all, ring, dz, wt_ref, r_ref, dc_ref, w_sem, ring_sem, out_sem, sem,
):
    depth = ring.shape[0]

    def gates_load(s, slot):
        at = pl.ds(pl.multiple_of((steps - 1 - s) * rows, rows), rows)
        return pltpu.make_async_copy(gates_hbm.at[layer, at, :], ring.at[slot], ring_sem.at[slot])

    def store(s):
        at = pl.ds(pl.multiple_of((steps - 1 - s) * rows, rows), rows)
        return pltpu.make_async_copy(dz.at[at, :], dz_out.at[at, :], out_sem)

    def e_step(t, col):
        first, count = col.start // 128, col.size // 128
        at = pl.ds(t, rows, stride=steps)
        return jnp.concatenate([e_all[first + i, at, :] for i in range(count)], axis=1)

    def w_load(k):
        cols = pl.ds(k * hidden, hidden)
        return pltpu.make_async_copy(w_hbm.at[layer, pl.ds(hidden, hidden), cols], w.at[:, cols], w_sem.at[k])

    tiles = hidden // 128
    loads = [pltpu.make_async_copy(c_hbm.at[layer], c_all, sem.at[tiles])]
    for i in range(tiles):
        loads.append(pltpu.make_async_copy(e_hbm.at[:, pl.ds(i * 128, 128)], e_all.at[i], sem.at[i]))
    for k in range(4):
        w_load(k).start()
    for load in loads:
        load.start()
    for s in range(min(depth, steps)):
        gates_load(s, s).start()
    r_ref[...] = jnp.zeros_like(r_ref)
    dc_ref[...] = jnp.zeros_like(dc_ref)
    db_ref[...] = jnp.zeros_like(db_ref)
    for k in range(4):
        w_load(k).wait()
        transpose_gate(hidden, k, w, wt_ref)
    for load in loads:
        load.wait()

    @pl.loop(0, steps)
    def _(s):
        t = steps - 1 - s
        slot = lax.rem(s, depth)
        gates_load(s, slot).wait()
        backward_step(
            rows, hidden, t, lambda col: ring[slot, :, col], lambda col: e_step(t, col),
            lambda at, col: c_all[at, col], wt_ref, r_ref, dc_ref, dz, db_ref,
        )

        @pl.when(s + depth < steps)
        def _():
            gates_load(s + depth, slot).start()

        @pl.when(s > 0)
        def _():
            store(s - 1).start()

    store(steps - 1).start()

    @pl.loop(0, steps)
    def _(s):
        store(s).wait()


def backward(layer, e_rows, w_stack, gates, c_all, rows):
    _, _, width = w_stack.shape
    hidden = width // 4
    total = e_rows.shape[0]
    steps = total // rows
    dma = pltpu.SemaphoreType.DMA
    return pl.pallas_call(
        functools.partial(backward_kernel, layer, rows, steps, hidden),
        in_specs=[pl.BlockSpec(memory_space=pl.ANY)] * 4,
        out_specs=[pl.BlockSpec(memory_space=pl.ANY), pl.BlockSpec(memory_space=pltpu.VMEM)],
        out_shape=[
            jax.ShapeDtypeStruct((total, width), jnp.bfloat16),
            jax.ShapeDtypeStruct((8, width), jnp.float32),
        ],
        scratch_shapes=[
            pltpu.VMEM((hidden // 128, total, 128), jnp.float32),
            pltpu.VMEM((hidden, width), jnp.bfloat16),
            pltpu.VMEM((total + rows, hidden), jnp.float32),
            pltpu.VMEM((4, rows, width), jnp.float32),
            pltpu.VMEM((total, width), jnp.bfloat16),
            pltpu.VMEM((width, hidden + PAD), jnp.bfloat16),
            pltpu.VMEM((rows, hidden), jnp.float32),
            pltpu.VMEM((rows, hidden), jnp.float32),
            dma((4,)), dma((4,)), dma, dma((hidden // 128 + 1,)),
        ],
        compiler_params=pltpu.CompilerParams(vmem_limit_bytes=VMEM_MAX),
        cost_estimate=pl.CostEstimate(
            flops=20 * 2 * total * hidden * width,
            bytes_accessed=2 * hidden * width + 7 * 4 * total * hidden,
            transcendentals=0,
        ),
        name=f"lstm_backward_{layer}",
    )(e_rows, w_stack, gates, c_all)


MESH = pl.DeviceIdType.MESH
ORDER = (7, 6, 5, 3, 4, 2, 1, 0)
AXES = ((0, 1, 2), (1, 2, 0), (2, 0, 1))


def colour_columns(width):
    tiles = width // 128
    first = -(-tiles // 3)
    second = -(-(tiles - first) // 2)
    sizes = (first * 128, second * 128, (tiles - first - second) * 128)
    return ((0, sizes[0]), (sizes[0], sizes[1]), (sizes[0] + sizes[1], sizes[2]))


def slot_one(code, axes):
    return ((code >> axes[1]) & 1) * 2 + ((code >> axes[2]) & 1)


def add_into(out_ref, a_ref, b_ref):
    @pl.loop(0, out_ref.shape[0] // 16)
    def _(i):
        at = pl.ds(pl.multiple_of(i * 16, 16), 16)
        out_ref[at, :] = a_ref[at, :] + b_ref[at, :]


def grads_kernel(layer, rows, hidden, dz_hbm, db_hbm, x_hbm, h_hbm, w_hbm, gates_hbm, c_hbm, *refs):
    below = layer - 1
    if layer:
        shard_ref, dbsum_ref, dz_out, db_ref, *refs = refs
        dz, uh, uht, w, p, r0, r1, r2, r3, db8, part_db, got_db, *refs = refs
        local_sem, s0, q0, s1, q1, s2, q2, s3, q3, sd, qd, *refs = refs
        dx_ref, c_all, ring, r_ref, dc_ref, ring_sem = refs
    else:
        shard_ref, dbsum_ref, dx_ref, *refs = refs
        dz, uh, uht, w, p, r0, r1, r2, r3, db8, part_db, got_db, *refs = refs
        local_sem, s0, q0, s1, q1, s2, q2, s3, q3, sd, qd = refs
    total, width = dz.shape
    steps = total // rows
    block = 2 * hidden // 16
    parts = width // hidden
    me = lax.axis_index("data")
    z = lax.axis_index("replica")
    y, x, c = me // 4, lax.rem(me // 2, 2), lax.rem(me, 2)
    partner = {"replica": z, "data": y * 4 + x * 2 + 1 - c}
    across = (
        {"replica": z, "data": y * 4 + (1 - x) * 2 + c},
        {"replica": z, "data": (1 - y) * 4 + x * 2 + c},
        {"replica": 1 - z, "data": me},
    )

    u_src = x_hbm if layer == 0 else h_hbm.at[below, pl.ds(rows, total), :]
    loads = [
        pltpu.make_async_copy(u_src, uh.at[:, pl.ds(0, hidden)], local_sem.at[0]),
        pltpu.make_async_copy(h_hbm.at[layer, pl.ds(0, total), :], uh.at[:, pl.ds(hidden, hidden)], local_sem.at[1]),
        pltpu.make_async_copy(dz_hbm, dz, local_sem.at[2]),
        pltpu.make_async_copy(db_hbm, db8, local_sem.at[3]),
        pltpu.make_async_copy(w_hbm.at[layer, pl.ds(0, hidden), :], w, local_sem.at[4]),
    ]
    if layer:
        loads.append(pltpu.make_async_copy(c_hbm.at[below], c_all, local_sem.at[5]))
    for load in loads:
        load.start()

    def gates_load(s, slot):
        at = pl.ds(pl.multiple_of((steps - 1 - s) * rows, rows), rows)
        return pltpu.make_async_copy(gates_hbm.at[below, at, :], ring.at[slot], ring_sem.at[slot])

    depth = 4
    if layer:
        for s in range(min(depth, steps)):
            gates_load(s, s).start()

    barrier = pltpu.get_barrier_semaphore()
    for device in (partner,) + across:
        pl.semaphore_signal(barrier, inc=1, device_id=device, device_id_type=MESH)
    pl.semaphore_wait(barrier, 4)

    def remote(src, dst, send_sem, recv_sem, device):
        return pltpu.make_async_remote_copy(
            src_ref=src, dst_ref=dst, send_sem=send_sem, recv_sem=recv_sem, device_id=device, device_id_type=MESH
        )

    columns = colour_columns(width)
    copies = {}
    for code in range(8):
        for n in range(parts):
            at = code * parts + n
            src = p.at[code, 1 - c, :, pl.ds(n * hidden, hidden)]
            copies[0, code, n] = remote(src, r0.at[pl.ds(at * block, block), pl.ds(0, hidden)], s0.at[at], q0.at[at], partner)
    for k, axes in enumerate(AXES):
        cols = pl.ds(*columns[k])
        for code in range(8):
            bits = [(code >> axis) & 1 for axis in axes]
            src = p.at[code, c, :, cols]
            if bits[0]:
                slot = slot_one(code, axes)
                at = k * 4 + slot
                copies[1, k, slot] = remote(src, r1.at[slot, :, cols], s1.at[at], q1.at[at], across[axes[0]])
            elif bits[1]:
                at = k * 2 + bits[2]
                copies[2, k, bits[2]] = remote(src, r2.at[bits[2], :, cols], s2.at[at], q2.at[at], across[axes[1]])
            elif bits[2]:
                copies[3, k] = remote(src, r3.at[:, cols], s3.at[k], q3.at[k], across[axes[2]])
    for stage, device in enumerate((partner,) + across):
        copies[4, stage] = remote(part_db.at[stage], got_db.at[stage], sd.at[stage], qd.at[stage], device)

    def bias_stage(stage):
        copies[4, stage].wait_recv()
        out = part_db.at[stage + 1] if stage < 3 else dbsum_ref
        out[...] = part_db[stage] + got_db[stage]
        if stage < 3:
            copies[4, stage + 1].start()

    loads[3].wait()
    part_db[0] = jnp.sum(db8[...], axis=0, keepdims=True).astype(jnp.bfloat16).astype(jnp.float32)
    loads[0].wait()
    loads[1].wait()

    @pl.loop(0, 2 * hidden // 128)
    def _(i):
        at = pl.ds(pl.multiple_of(i * 128, 128), 128)
        uht[at, :] = uh[:, at].T

    copies[4, 0].start()
    loads[2].wait()
    chunk = min(width, 1024)

    def receive_partner(code):
        for n in range(parts):
            copies[0, code, n].wait_recv()
            cols = pl.ds(n * hidden, hidden)
            mine = p.at[code, c, :, cols]
            add_into(mine, mine, r0.at[pl.ds((code * parts + n) * block, block), pl.ds(0, hidden)])
        for k, axes in enumerate(AXES):
            if (code >> axes[0]) & 1:
                copies[1, k, slot_one(code, axes)].start()

    before = None
    for code in ORDER:
        sides = [
            own + flip - 2 * own * flip
            for own, flip in ((z, (code >> 2) & 1), (y, (code >> 1) & 1), (x, code & 1))
        ]
        base = pl.multiple_of(((sides[0] * 2 + sides[1]) * 2 + sides[2]) * 2 * block, 2 * block)

        @pl.loop(0, width // chunk)
        def _(n):
            cols = pl.ds(pl.multiple_of(n * chunk, chunk), chunk)
            part = jnp.dot(uht[pl.ds(base, 2 * block), :], dz[:, cols], preferred_element_type=jnp.float32)
            low = part.astype(jnp.bfloat16)
            p[code, 0, :, cols] = low[:block]
            p[code, 1, :, cols] = low[block:]

        if before is not None:
            receive_partner(before)
        for n in range(parts):
            copies[0, code, n].start()
        before = code
    receive_partner(before)
    bias_stage(0)

    loads[4].wait()
    step = BLK

    @pl.loop(0, hidden // step)
    def _(n):
        at = pl.ds(pl.multiple_of(n * step, step), step)
        dx_ref[:, at] = lax.dot_general(
            dz[...], w[at, :], (((1,), (1,)), ((), ())), preferred_element_type=jnp.float32
        )

    def first_crossing(codes):
        for code in codes:
            for k, axes in enumerate(AXES):
                if (code >> axes[0]) & 1:
                    slot = slot_one(code, axes)
                    cols = pl.ds(*columns[k])
                    copies[1, k, slot].wait_recv()
                    here = code ^ (1 << axes[0])
                    mine = p.at[here, c, :, cols]
                    add_into(mine, mine, r1.at[slot, :, cols])
                    if (here >> axes[1]) & 1:
                        copies[2, k, (here >> axes[2]) & 1].start()

    def second_crossing(bit):
        for k, axes in enumerate(AXES):
            cols = pl.ds(*columns[k])
            copies[2, k, bit].wait_recv()
            mine = p.at[bit << axes[2], c, :, cols]
            add_into(mine, mine, r2.at[bit, :, cols])
            if bit:
                copies[3, k].start()

    bias_stage(1)
    if layer:
        reload = pltpu.make_async_copy(w_hbm.at[below, pl.ds(hidden, hidden), :], w, local_sem.at[4])
        reload.start()
        r_ref[...] = jnp.zeros_like(r_ref)
        dc_ref[...] = jnp.zeros_like(dc_ref)
        db_ref[...] = jnp.zeros_like(db_ref)
        loads[5].wait()
        reload.wait()
        first_crossing(ORDER[:1])
        for k in range(4):
            transpose_gate(hidden, k, w, r0)

        @pl.loop(0, steps)
        def _(s):
            t = steps - 1 - s
            slot = lax.rem(s, depth)
            gates_load(s, slot).wait()
            now = pl.ds(pl.multiple_of(t * rows, rows), rows)
            backward_step(
                rows, hidden, t, lambda col: ring[slot, :, col], lambda col: dx_ref[now, col],
                lambda at, col: c_all[at, col], r0, r_ref, dc_ref, dz, db_ref,
            )

            @pl.when(s + depth < steps)
            def _():
                gates_load(s + depth, slot).start()

            @pl.when(s == steps // 16)
            def _():
                first_crossing(ORDER[1:4])

            @pl.when(s == steps // 4)
            def _():
                first_crossing(ORDER[4:])

            @pl.when(s == steps // 2)
            def _():
                second_crossing(1)

            @pl.when(s == steps - 3)
            def _():
                second_crossing(0)

        store = pltpu.make_async_copy(dz, dz_out, local_sem.at[2])
        store.start()
    else:
        first_crossing(ORDER)
        second_crossing(1)
        second_crossing(0)
    bias_stage(2)
    bias_stage(3)
    for k in range(3):
        cols = pl.ds(*columns[k])
        copies[3, k].wait_recv()
        add_into(shard_ref.at[:, cols], p.at[0, c, :, cols], r3.at[:, cols])
    for copy in copies.values():
        copy.wait_send()
    if layer:
        store.wait()


def grads(layer, dz, db, x_rows, h_all, w_stack, gates, c_all, rows):
    total, width = dz.shape
    hidden = width // 4
    block = 2 * hidden // 16
    parts = 8 * (width // hidden)
    dma = pltpu.SemaphoreType.DMA
    vmem = pl.BlockSpec(memory_space=pltpu.VMEM)
    hbm = pl.BlockSpec(memory_space=pl.ANY)
    out_shape = [
        jax.ShapeDtypeStruct((block, width), jnp.bfloat16),
        jax.ShapeDtypeStruct((1, width), jnp.float32),
    ]
    scratch = [
        pltpu.VMEM((total, width), jnp.bfloat16),
        pltpu.VMEM((total, 2 * hidden), jnp.bfloat16),
        pltpu.VMEM((2 * hidden, total), jnp.bfloat16),
        pltpu.VMEM((hidden, width), jnp.bfloat16),
        pltpu.VMEM((8, 2, block, width), jnp.bfloat16),
        pltpu.VMEM((width, hidden + PAD), jnp.bfloat16),
        pltpu.VMEM((4, block, width), jnp.bfloat16),
        pltpu.VMEM((2, block, width), jnp.bfloat16),
        pltpu.VMEM((block, width), jnp.bfloat16),
        pltpu.VMEM((8, width), jnp.float32),
        pltpu.VMEM((4, 1, width), jnp.float32),
        pltpu.VMEM((4, 1, width), jnp.float32),
        dma((6,)), dma((parts,)), dma((parts,)), dma((12,)), dma((12,)), dma((6,)), dma((6,)), dma((3,)), dma((3,)),
        dma((4,)), dma((4,)),
    ]
    if layer:
        out_specs = [vmem, vmem, hbm, vmem]
        out_shape += [
            jax.ShapeDtypeStruct((total, width), jnp.bfloat16),
            jax.ShapeDtypeStruct((8, width), jnp.float32),
        ]
        scratch += [
            pltpu.VMEM((total, hidden), jnp.float32),
            pltpu.VMEM((total + rows, hidden), jnp.float32),
            pltpu.VMEM((4, rows, width), jnp.float32),
            pltpu.VMEM((rows, hidden), jnp.float32),
            pltpu.VMEM((rows, hidden), jnp.float32),
            dma((4,)),
        ]
    else:
        out_specs = [vmem, vmem, vmem]
        out_shape += [jax.ShapeDtypeStruct((total, hidden), jnp.float32)]
    return pl.pallas_call(
        functools.partial(grads_kernel, layer, rows, hidden),
        in_specs=[hbm] * 7,
        out_specs=out_specs,
        out_shape=out_shape,
        scratch_shapes=scratch,
        compiler_params=pltpu.CompilerParams(
            collective_id=layer, has_side_effects=True, vmem_limit_bytes=VMEM_MAX
        ),
        cost_estimate=pl.CostEstimate(
            flops=6 * total * hidden * width * 5, bytes_accessed=8 * hidden * width, transcendentals=0
        ),
        name=f"lstm_grads_{layer}",
    )(dz, db, x_rows, h_all, w_stack, gates, c_all)


def widen_kernel(part_ref, *refs):
    refs[-1][0] = part_ref[...].astype(jnp.float32)


def widen(total, part, layer, layers):
    height, width = part.shape
    block = min(height, 256)
    return pl.pallas_call(
        widen_kernel,
        grid=(height // block,),
        in_specs=[pl.BlockSpec((block, width), lambda i: (i, 0))]
        + ([] if total is None else [pl.BlockSpec(memory_space=pl.ANY)]),
        out_specs=pl.BlockSpec((1, block, width), lambda i: (layer, i, 0)),
        out_shape=jax.ShapeDtypeStruct((layers, height, width), jnp.float32),
        input_output_aliases={} if total is None else {1: 0},
        cost_estimate=pl.CostEstimate(flops=height * width, bytes_accessed=6 * height * width, transcendentals=0),
        name=f"widen_{layer}",
    )(*([part] if total is None else [part, total]))


def solution(mesh):
    batch_axes = ("replica", "data")

    def local_grads(x_loc, dy_loc, w_stack, b_stack):
        layers, _, width = w_stack.shape
        hidden = width // 4
        rows, steps, _ = x_loc.shape
        x_rows = jnp.swapaxes(x_loc, 0, 1).reshape(steps * rows, hidden)
        e_rows = dy_loc.reshape(rows * steps, hidden)
        h_all, gates, c_all = forward(x_rows, w_stack, b_stack, rows)
        db_list = []
        gathered = []
        dz, db = backward(layers - 1, e_rows, w_stack, gates, c_all, rows)
        for layer in reversed(range(layers)):
            shard, db_sum, *rest = grads(layer, dz, db, x_rows, h_all, w_stack, gates, c_all, rows)
            if layer:
                dz, db = rest
            db_list.append(db_sum)
            gathered.append((layer, lax.all_gather(shard, batch_axes, axis=0, tiled=True)))
        e_rows = rest[0]
        db_sum = jnp.concatenate(db_list[::-1], axis=0)
        dw_sum = None
        for layer, summed in gathered:
            if dw_sum is None:
                summed, e_rows = lax.optimization_barrier((summed, e_rows))
            else:
                summed, dw_sum = lax.optimization_barrier((summed, dw_sum))
            dw_sum = widen(dw_sum, summed, layer, layers)
        dx = jnp.swapaxes(e_rows.reshape(steps, rows, hidden), 0, 1)
        return dw_sum, db_sum, dx

    return jax.shard_map(
        local_grads,
        mesh=mesh,
        in_specs=(P(batch_axes), P(batch_axes), P(), P()),
        out_specs=(P(), P(), P(batch_axes)),
        check_vma=False,
    )
```
